512 devices in a mesh: gx: 8 (over x, core), gy: 64 (over y, z).
Axes of the slice: x: 4, y: 8, z: 8, core: 2. Of those that a mesh axis runs over, the one named last changes fastest.
Arguments:
- cell: int32 [16777216], P(('gx', 'gy')), may hold values from 0 to 524287
- vehicle: int32 [16777216], P(('gx', 'gy')), may hold values from 0 to 1023
- speed: float32 [16777216], P(('gx', 'gy')), may hold values from 0 to 64, as said below
Outputs:
- top_speed: float32 [524288], P(('gx', 'gy'))
- top_vehicle: int32 [524288], P(('gx', 'gy'))
The draws below stay inside these ranges and needn't reach their ends.
Inputs may be any that keep to these rules, and one draw needn't show every extreme that they name: Every speed is a whole multiple of 1/1024.
All inputs are finite; a program needn't handle non-finite values.
Results may differ from the reference program's by a relative error of at most 0.0003.
Values sent between devices are 32-bit elements; how exact they have to be, the bound alone decides.
A program may use at most 64 MiB of HBM per device.

```python
import math
import jax
import jax.numpy as jnp
import numpy as np

CELLS = 524288
VEHICLES = 1024
EVENTS = 16777216


def draw_speed(key, part):
    level_key = jax.random.fold_in(key, 11)
    plant_key = jax.random.fold_in(key, 23)
    levels = jax.random.randint(level_key, (EVENTS,), 0, 65537)
    values = levels.astype(jnp.float32) / 1024.0
    planted = jax.random.randint(plant_key, (EVENTS,), 0, 512)
    values = jnp.where(planted == 0, 64.0, values)
    return values.astype(jnp.float32)


def with_ends(entries, own_key, least, high):
    dims = entries.shape
    index_at = [jax.random.randint(jax.random.fold_in(own_key, axis), (), 0, dims[axis]) for axis in range(len(dims))]
    entries = entries.at[tuple(index_at)].set(least)
    longest = dims.index(max(dims))
    index_at[longest] = (index_at[longest] + 1) % dims[longest]
    return entries.at[tuple(index_at)].set(high)


def ranked_wide(own_key, extent, amount, slope):
    weights = [min(1 << octave, amount + 1 - (1 << octave)) * (1 << 20) // math.isqrt((1 << octave) ** slope) + 1 for octave in range((amount + 1).bit_length()) if 1 << octave <= amount]
    scale = 1 + sum(weights) // (1 << 30)
    listing = np.cumsum(np.array([max(1, weight // scale) for weight in weights]))
    ticket = jax.random.randint(jax.random.fold_in(own_key, 1), extent, 0, int(listing[len(weights) - 1]))
    start = jnp.left_shift(1, jnp.searchsorted(jnp.asarray(listing, jnp.int32), ticket, side="right").astype(jnp.int32))
    rank = start - 1 + jax.random.randint(jax.random.fold_in(own_key, 4), extent, 0, 1 << 30) % jnp.minimum(start, amount + 1 - start)
    return jax.random.permutation(jax.random.fold_in(own_key, 2), amount)[rank].astype(jnp.int32)


def setup_inputs(seed: int = 0) -> dict:
    splits = jax.random.split(jax.random.key(seed), 4)
    cell = with_ends(ranked_wide(splits[0], (EVENTS,), CELLS, 2), jax.random.fold_in(splits[0], 3), 0, CELLS - 1).astype(jnp.int32)
    vehicle = with_ends(jax.random.randint(splits[1], (EVENTS,), 0, VEHICLES), jax.random.fold_in(splits[1], 1), 0, VEHICLES - 1).astype(jnp.int32)
    speed = draw_speed(jax.random.fold_in(splits[3], 71), 0)
    return dict(cell=cell, vehicle=vehicle, speed=speed)


def reference(cell, vehicle, speed):
    top_speed = jnp.full((CELLS,), -1.0, jnp.float32).at[cell].max(speed)
    chosen = jnp.where(speed == top_speed[cell], vehicle, VEHICLES).astype(jnp.int32)
    lowest = jnp.full((CELLS,), VEHICLES, jnp.int32).at[cell].min(chosen)
    top_vehicle = jnp.where(lowest < VEHICLES, lowest, -1).astype(jnp.int32)
    return top_speed, top_vehicle
```

```python
import jax
import jax.numpy as jnp
import numpy as np
from jax import lax
from jax.experimental import pallas as pl
from jax.experimental.pallas import tpu as pltpu
from jax.sharding import PartitionSpec as P

CELLS = 524288
VEHICLES = 1024
MESH = pl.DeviceIdType.MESH
SIGN = np.int32(-(2**31))
CAP = 2048
EMPTY = 131072


def swapped(block, axis, apart):
    count = lax.axis_size(axis)
    route = []
    for low in range(count):
        high = low | 1 << apart
        if high != low and high < count:
            route += [(low, high), (high, low)]
    return lax.ppermute(block, axis, route)


def combine(first, second):
    speed_a = first[0]
    speed_b = second[0]
    best = jnp.maximum(speed_a, speed_b)
    ident = jnp.where(
        speed_a > speed_b,
        first[1],
        jnp.where(speed_b > speed_a, second[1], jnp.minimum(first[1], second[1])),
    )
    return jnp.stack([best, ident])


def dense_path(cell, vehicle, speed):
    local_best = jnp.full((CELLS,), -1.0, jnp.float32).at[cell].max(speed)
    chosen = jnp.where(speed == local_best[cell], vehicle, VEHICLES)
    local_ident = jnp.full((CELLS,), VEHICLES, jnp.int32).at[cell].min(chosen)
    paired = jnp.stack([local_best, local_ident.astype(jnp.float32)])
    outer = lax.axis_size("gx")
    inner = lax.axis_size("gy")
    nbits = (outer * inner).bit_length() - 1
    myself = lax.axis_index(("gx", "gy"))
    buffer = paired
    for level in reversed(range(nbits)):
        half = buffer.shape[1] // 2
        side = myself >> level & 1
        keep = lax.dynamic_slice_in_dim(buffer, side * half, half, 1)
        give = lax.dynamic_slice_in_dim(buffer, (1 - side) * half, half, 1)
        partner = swapped(give, ("gx", "gy"), level)
        buffer = combine(keep, partner)
    best = buffer[0]
    lowest = buffer[1].astype(jnp.int32)
    return best, jnp.where(lowest < VEHICLES, lowest, -1)


def lanes():
    return lax.broadcasted_iota(jnp.int32, (8, 128), 1)


def subs():
    return lax.broadcasted_iota(jnp.int32, (8, 128), 0)


def lane_xor(x, index):
    return jnp.take_along_axis(x, index, axis=1)


def sub_xor(x, bit):
    d = 1 << bit
    if d == 4:
        return pltpu.roll(x, 4, 0)
    return jnp.where((subs() & d) != 0, pltpu.roll(x, d, 0), pltpu.roll(x, 8 - d, 0))


def above(c1, k1, c2, k2):
    return (c1 > c2) | ((c1 == c2) & (k1 > k2))


def order_pair(a, b, down):
    swap = above(*a, *b)
    if down is True:
        a, b = b, a
    elif down is not False:
        swap = swap ^ down
    low = tuple(jnp.where(swap, y, x) for x, y in zip(a, b))
    high = tuple(jnp.where(swap, x, y) for x, y in zip(a, b))
    return low, high


def order_cross(x, y, wants_max):
    swap = above(*x, *y) ^ wants_max
    return tuple(jnp.where(swap, q, p) for p, q in zip(x, y))


def move_pair(a, b, bit):
    mask = SIGN | np.int32(1 << bit)
    one = mask
    ma, mb = a[0] & mask, b[0] & mask
    a0, b0 = ma == SIGN, mb == SIGN
    a1, b1 = ma == one, mb == one
    low = (jnp.where(b0, b[0], jnp.where(a0, a[0], 0)), jnp.where(b0, b[1], a[1]))
    high = (jnp.where(a1, a[0], jnp.where(b1, b[0], 0)), jnp.where(a1, a[1], b[1]))
    return low, high


def move_cross(x, y, bit, here):
    mask = SIGN | np.int32(1 << bit)
    mx, my = (x[0] & mask) == here, (y[0] & mask) == here
    return jnp.where(my, y[0], jnp.where(mx, x[0], 0)), jnp.where(my, y[1], x[1])


def get(refs, v):
    return refs[0][v], refs[1][v]


def put(refs, v, pair):
    refs[0][v] = pair[0]
    refs[1][v] = pair[1]


def register_steps(refs, group_bits, count, bits, step):
    for base in range(count):
        if any(base >> b & 1 for b in group_bits):
            continue
        members = [base]
        for b in group_bits:
            members += [m | 1 << b for m in members]
        held = {m: get(refs, m) for m in members}
        for b in bits:
            for m in members:
                if not m >> b & 1:
                    held[m], held[m | 1 << b] = step(held[m], held[m | 1 << b], b, m)
        for m in members:
            put(refs, m, held[m])


def cross_steps(refs, count, steps):
    for step in steps:
        for v in range(count):
            put(refs, v, step(get(refs, v), v))


def batcher(n):
    pairs = []

    def merge(lo, n, r):
        m = r * 2
        if m < n:
            merge(lo, n, m)
            merge(lo + r, n, m)
            for i in range(lo + r, lo + n - r, m):
                pairs.append((i, i + r))
        else:
            pairs.append((lo, lo + r))

    def sort(lo, n):
        if n > 1:
            m = n // 2
            sort(lo, m)
            sort(lo + m, m)
            merge(lo, n, 1)

    sort(0, n)
    return pairs


def total(x):
    s = jnp.sum(x.astype(jnp.float32), axis=0, keepdims=True)
    s = jnp.sum(s, axis=1, keepdims=True)
    return jnp.broadcast_to(s, (8, 128)).astype(jnp.int32)


def xor_prefix(x, order):
    lane, sub = lanes(), subs()
    before, block = jnp.zeros_like(x), x
    for kind, i in order:
        if kind == "s":
            other, bit = sub_xor(block, i), (sub >> i) & 1
        else:
            other, bit = lane_xor(block, lane ^ (1 << i)), (lane >> i) & 1
        before = before + jnp.where(bit == 1, other, 0)
        block = block + other
    return before, block


def sort_events(cell, vehicle, speed, A, B):
    lane, sub = lanes(), subs()
    R = (A, B)
    flip = -(sub & 1)
    held = []
    for v in range(32):
        c = cell[v]
        c = (
            (c & 0x7E000 | ((c >> 10) & 1))
            | ((c & 0x1800) | ((c & 7) << 8))
            | (((c >> 2) & 0xE0) | ((c >> 2) & 0x1E))
        )
        k = (speed[v] * 1024.0).astype(jnp.int32) * 1024 + (1023 - vehicle[v])
        held.append((c ^ flip, k ^ flip))
    for i, j in batcher(32):
        held[i], held[j] = order_pair(held[i], held[j], False)
    for v in range(32):
        put(R, v, (held[v][0] ^ flip, held[v][1] ^ flip))

    def tail(down):
        register_steps(R, (3, 4), 32, (4, 3), lambda a, b, *_: order_pair(a, b, down))
        register_steps(R, (0, 1, 2), 32, (2, 1, 0), lambda a, b, *_: order_pair(a, b, down))

    def sub_step(i, down):
        wants = (((sub >> i) & 1) == 1) ^ down
        return lambda x, v: order_cross(x, (sub_xor(x[0], i), sub_xor(x[1], i)), wants)

    for top in (1, 2, 3):
        down = ((sub >> top) & 1) == 1 if top < 3 else (lane & 1) == 1
        cross_steps(R, 32, [sub_step(i, down) for i in reversed(range(top))])
        tail(down)

    def stage(s, _):
        turned = (lane >> (s + 1)) & 1
        down = turned == 1

        def lane_step(n, _):
            i = s - n
            index = lane ^ (1 << i)
            wants = (((lane >> i) & 1) ^ turned) == 1
            cross_steps(
                R, 32, [lambda x, v: order_cross(x, (lane_xor(x[0], index), lane_xor(x[1], index)), wants)]
            )
            return 0

        lax.fori_loop(0, s + 1, lane_step, 0)
        cross_steps(R, 32, [sub_step(i, down) for i in (2, 1, 0)])
        tail(down)
        return 0

    lax.fori_loop(0, 7, stage, 0)


def list_rank(v):
    lane = lanes()
    return (v >> 1) * CAP + ((lane & 7) << 8) + (subs() << 5) + ((lane >> 3) << 1) + (v & 1)


LIST_BITS = [("v", 0), ("l", 3), ("l", 4), ("l", 5), ("l", 6), ("s", 0), ("s", 1), ("s", 2), ("l", 0), ("l", 1), ("l", 2),
             ("v", 1), ("v", 2), ("v", 3)]


def route(refs, count, order, shift=16):
    lane, sub = lanes(), subs()
    at = 0
    while at < len(order):
        bit, kind, i = order[at]
        if kind == "v":
            run = [order[at]]
            while at + len(run) < len(order) and order[at + len(run)][1] == "v" and len(run) < 3:
                run.append(order[at + len(run)])
            number = {i: shift + b for b, _, i in run}
            register_steps(
                refs, tuple(i for _, _, i in run), count, tuple(i for _, _, i in run),
                lambda a, b, i, _: move_pair(a, b, number[i]),
            )
            at += len(run)
            continue
        b = shift + bit
        if kind == "s":
            here = SIGN | (((sub >> i) & 1) << b)
            step = lambda x, v: move_cross(x, (sub_xor(x[0], i), sub_xor(x[1], i)), b, here)
        else:
            here = SIGN | (((lane >> i) & 1) << b)
            index = lane ^ (1 << i)
            step = lambda x, v: move_cross(x, (lane_xor(x[0], index), lane_xor(x[1], index)), b, here)
        cross_steps(refs, count, [step])
        at += 1


def group_starts(groups, valid, count):
    starts = [jnp.zeros((8, 128), jnp.int32)]
    for j in range(1, 9):
        t = jnp.zeros((8, 128), jnp.int32)
        for v in range(count):
            t = t + jnp.where(valid[v] & (groups[v] < j), 1, 0)
        starts.append(total(t))
    return starts


def crowded(starts):
    most = jnp.zeros((8, 128), jnp.int32)
    for j in range(8):
        most = jnp.maximum(most, starts[j + 1] - starts[j])
    return (most > CAP).astype(jnp.int32)


def offsets(groups, starts):
    moved = jnp.zeros((8, 128), jnp.int32)
    for j in range(1, 8):
        moved = jnp.where(groups == j, j * CAP - starts[j], moved)
    return moved


def compact_events(A, B, S, T):
    lane, sub = lanes(), subs()
    first = A[0]
    down1 = pltpu.roll(first, 7, 0)
    follow = jnp.where(sub == 7, pltpu.roll(down1, 127, 1), down1)
    last = (sub == 7) & (lane == 127)
    run = jnp.zeros((8, 128), jnp.int32)
    keeps, ranks = [], []
    cells = [A[v] for v in range(32)]
    for v in range(32):
        nxt = cells[v + 1] if v < 31 else follow
        keep = cells[v] != nxt
        if v == 31:
            keep = keep | last
        keeps.append(keep)
        ranks.append(run)
        run = run + keep.astype(jnp.int32)
    before, every = xor_prefix(run, [("s", 0), ("s", 1), ("s", 2)] + [("l", i) for i in range(7)])
    for v in range(32):
        c = cells[v]
        w1 = SIGN | ((before + ranks[v]) << 16) | (c & 0xFFFF)
        A[v] = jnp.where(keeps[v], w1, 0)
        B[v] = B[v] | ((c >> 16) << 27)
    order = [(i, "v", i) for i in range(5)] + [(5 + i, "s", i) for i in range(3)] + [(8 + i, "l", i) for i in range(7)]
    route((A, B), 32, order)
    low = lane < 64
    for v in range(16):
        for X, Y in ((A, S), (B, T)):
            Y[v] = jnp.where(low, X[v], pltpu.roll(X[v + 16], 64, 1))
    for j in range(3):
        d = 8 << j
        bit = (lane & d) != 0
        for v in range(16):
            w = v | 2 << j
            if w == v:
                continue
            for Y in (S, T):
                a, b = Y[v], Y[w]
                Y[v] = jnp.where(bit, pltpu.roll(b, d, 1), a)
                Y[w] = jnp.where(bit, b, pltpu.roll(a, 128 - d, 1))
    valid = [S[v] < 0 for v in range(16)]
    groups = [T[v] >> 27 for v in range(16)]
    starts = group_starts(groups, valid, 16)
    flag = crowded(starts) | (every > 8 * CAP).astype(jnp.int32)
    for v in range(16):
        target = list_rank(v) + offsets(groups[v], starts)
        S[v] = jnp.where(valid[v], SIGN | (target << 16) | (S[v] & 0xFFFF), 0)
        T[v] = T[v] & 0x7FFFFFF
    return flag


def expand_lists(S, T):
    route((S, T), 16, [(b, *LIST_BITS[b]) for b in reversed(range(14))])


def pack_messages(S, T, out):
    for v in range(16):
        g, h = v >> 1, v & 1
        w, k = S[v], T[v]
        out[g, h] = jnp.where(w < 0, w & 0xFFFF, EMPTY).astype(jnp.float32)
        out[g, 2 + h] = (k >> 10).astype(jnp.float32) * (1.0 / 1024.0)
        out[g, 4 + h] = (1023 - (k & 1023)).astype(jnp.float32)


def key_of(speed, vehicle):
    return (speed * 1024.0).astype(jnp.int32) * 1024 + (1023 - vehicle.astype(jnp.int32))


def merge_lists(inbox, S, T):
    lane, sub = lanes(), subs()
    back = 127 - lane
    R = (S, T)
    for s in range(8):
        for h in range(2):
            pair = (inbox[s, h].astype(jnp.int32), key_of(inbox[s, 2 + h], inbox[s, 4 + h]))
            if s & 1:
                pair = tuple(lane_xor(sub_xor(sub_xor(sub_xor(x, 0), 1), 2), back) for x in pair)
                put(R, 2 * s + 1 - h, pair)
            else:
                put(R, 2 * s + h, pair)
    for level in (1, 2, 3):
        down = (lambda v: bool(v >> (level + 1) & 1)) if level < 3 else (lambda v: False)
        bits = tuple(reversed(range(1, level + 1)))
        register_steps(R, bits, 16, bits, lambda a, b, i, m: order_pair(a, b, down(m)))
        for kind, i in reversed(LIST_BITS[1:11]):
            if kind == "s":
                wants = {False: ((sub >> i) & 1) == 1, True: ((sub >> i) & 1) == 0}
                step = lambda x, v: order_cross(x, (sub_xor(x[0], i), sub_xor(x[1], i)), wants[down(v)])
            else:
                wants = {False: ((lane >> i) & 1) == 1, True: ((lane >> i) & 1) == 0}
                index = lane ^ (1 << i)
                step = lambda x, v: order_cross(x, (lane_xor(x[0], index), lane_xor(x[1], index)), wants[down(v)])
            cross_steps(R, 16, [step])
        register_steps(R, (0,), 16, (0,), lambda a, b, i, m: order_pair(a, b, down(m)))


def regroup(S, T):
    cells = [S[v] for v in range(16)]
    valid = [c < EMPTY for c in cells]
    groups = [c >> 13 for c in cells]
    starts = group_starts(groups, valid, 16)
    for v in range(16):
        target = list_rank(v) + offsets(groups[v], starts)
        S[v] = jnp.where(valid[v], SIGN | (target << 16) | (cells[v] & 0x1FFF), 0)
    flag = crowded(starts)
    expand_lists(S, T)
    return flag


def to_table(S, T):
    lane, sub = lanes(), subs()
    cells = [S[v] for v in range(16)]
    keeps = []
    for p in range(8):
        even, odd = cells[2 * p], cells[2 * p + 1]
        keeps.append((even != odd) & (even < EMPTY))
        ahead = pltpu.roll(even, 120, 1)
        wrapped = pltpu.roll(ahead, 7, 0)
        carried = pltpu.roll(wrapped, 127, 1)
        if p < 7:
            entry = jnp.broadcast_to(cells[2 * p + 2][0:1, 0:1], (8, 128))
            carried = jnp.where((lane & 7) == 7, entry, carried)
        nxt = jnp.where(lane >= 120, jnp.where(sub == 7, carried, wrapped), ahead)
        keep = odd != nxt
        if p == 7:
            keep = keep | ((lane == 127) & (sub == 7))
        keeps.append(keep & (odd < EMPTY))
    done = jnp.zeros((8, 128), jnp.int32)
    order = [("l", 3), ("l", 4), ("l", 5), ("l", 6), ("s", 0), ("s", 1), ("s", 2), ("l", 0), ("l", 1), ("l", 2)]
    for p in range(8):
        even, odd = (keeps[2 * p + h].astype(jnp.int32) for h in range(2))
        before, block = xor_prefix(even + odd, order)
        before = before + done
        done = done + block
        S[2 * p] = jnp.where(keeps[2 * p], SIGN | (before << 16) | cells[2 * p], 0)
        S[2 * p + 1] = jnp.where(keeps[2 * p + 1], SIGN | ((before + even) << 16) | cells[2 * p + 1], 0)
    route((S, T), 16, [(b, *LIST_BITS[b]) for b in range(14)])
    for v in range(8):
        w = S[v]
        S[v] = jnp.where(w < 0, SIGN | ((w & 0x1FFF) << 16), 0)
    route((S, T), 8, [(b, *LIST_BITS[b]) for b in reversed(range(13))])


def exchange_kernel(cell, vehicle, speed, best, ident, flags, A, B, S, T, out1, in1, out2, in2, out3, in3, mark, marks1,
                    mark2, marks2, send, recv):
    gx, gy = lax.axis_index("gx"), lax.axis_index("gy")
    y, z = gy // 8, gy % 8

    def peer(phase, j):
        if phase == 0:
            return (gx ^ j, gy)
        if phase == 1:
            return (gx, (y ^ j) * 8 + z)
        return (gx, y * 8 + (z ^ j))

    barrier = pltpu.get_barrier_semaphore()
    for phase in range(3):
        for j in range(1, 8):
            pl.semaphore_signal(barrier, inc=1, device_id=peer(phase, j), device_id_type=MESH)

    def copies(lane_of, phase, source, target):
        made = []
        for j in range(1, 8):
            made.append(
                pltpu.make_async_remote_copy(
                    src_ref=source(j),
                    dst_ref=target.at[j],
                    send_sem=send.at[lane_of, j],
                    recv_sem=recv.at[lane_of, j],
                    device_id=peer(phase, j),
                    device_id_type=MESH,
                )
            )
        return made

    sort_events(cell, vehicle, speed, A, B)
    flag = compact_events(A, B, S, T)
    expand_lists(S, T)
    pack_messages(S, T, out1)
    pl.semaphore_wait(barrier, 21)
    first = copies(0, 0, lambda j: out1.at[gx ^ j], in1)
    for c in first:
        c.start()
    in1[0] = out1[gx]
    for c in first:
        c.wait_recv()

    merge_lists(in1, S, T)
    flag = flag | regroup(S, T)
    mark[...] = flag.astype(jnp.float32)
    pack_messages(S, T, out2)
    second = copies(1, 1, lambda j: out2.at[y ^ j], in2)
    for c in second:
        c.start()
    flags1 = copies(2, 0, lambda j: mark, marks1)
    for c in flags1:
        c.start()
    in2[0] = out2[y]
    for c in flags1:
        c.wait_recv()
    seen = mark[...]
    for j in range(1, 8):
        seen = jnp.maximum(seen, marks1[j])
    mark2[...] = seen
    flags2 = copies(3, 1, lambda j: mark2, marks2)
    for c in flags2:
        c.start()
    for c in second:
        c.wait_recv()

    merge_lists(in2, S, T)
    to_table(S, T)
    for c in flags2:
        c.wait_recv()
    for j in range(1, 8):
        seen = jnp.maximum(seen, marks2[j])
    for v in range(8):
        there, k = S[v] < 0, T[v]
        out3[v, 0] = jnp.where(there, (k >> 10).astype(jnp.float32) * (1.0 / 1024.0), -1.0)
        out3[v, 1] = jnp.where(there, (1023 - (k & 1023)).astype(jnp.float32), 1024.0)
        out3[v, 2] = seen
    third = copies(4, 2, lambda j: out3.at[z ^ j], in3)
    for c in third:
        c.start()
    in3[0] = out3[z]
    for c in third:
        c.wait_recv()
    k = key_of(in3[0, 0], in3[0, 1])
    for j in range(1, 8):
        k = jnp.maximum(k, key_of(in3[j, 0], in3[j, 1]))
        seen = jnp.maximum(seen, in3[j, 2])
    best[...] = jnp.where(k < 0, -1.0, (k >> 10).astype(jnp.float32) * (1.0 / 1024.0))
    ident[...] = jnp.where(k < 0, -1, 1023 - (k & 1023))
    flags[...] = seen
    for group in (first, second, flags1, flags2, third):
        for c in group:
            c.wait_send()


def words(*shape):
    return pltpu.VMEM(shape + (8, 128), jnp.float32)


def sparse_path(cell, vehicle, speed):
    whole = pl.BlockSpec(memory_space=pltpu.VMEM)
    ints = lambda n: pltpu.VMEM((n, 8, 128), jnp.int32)
    return pl.pallas_call(
        exchange_kernel,
        out_shape=(
            jax.ShapeDtypeStruct((8, 128), jnp.float32),
            jax.ShapeDtypeStruct((8, 128), jnp.int32),
            jax.ShapeDtypeStruct((8, 128), jnp.float32),
        ),
        in_specs=[whole] * 3,
        out_specs=(whole,) * 3,
        scratch_shapes=[
            ints(32), ints(32), ints(16), ints(16),
            words(8, 6), words(8, 6), words(8, 6), words(8, 6), words(8, 3), words(8, 3),
            words(), words(8), words(), words(8),
            pltpu.SemaphoreType.DMA((5, 8)),
            pltpu.SemaphoreType.DMA((5, 8)),
        ],
        compiler_params=pltpu.CompilerParams(collective_id=0, has_side_effects=True),
    )(cell, vehicle, speed)


def per_device(cell, vehicle, speed):
    shaped = [x.reshape(32, 8, 128) for x in (cell, vehicle, speed)]
    best, ident, flags = sparse_path(*shaped)
    return lax.cond(
        flags[0, 0] > 0.0,
        lambda: dense_path(cell, vehicle, speed),
        lambda: (best.reshape(1024), ident.reshape(1024)),
    )


def solution(mesh):
    placed = (P(("gx", "gy")), P(("gx", "gy")), P(("gx", "gy")))
    return jax.shard_map(
        per_device,
        mesh=mesh,
        in_specs=placed,
        out_specs=(P(("gx", "gy")), P(("gx", "gy"))),
        check_vma=False,
    )
```

```python
import jax
import jax.numpy as jnp
import numpy as np
from jax import lax
from jax.experimental import pallas as pl
from jax.experimental.pallas import tpu as pltpu
from jax.sharding import PartitionSpec as P

CELLS = 524288
VEHICLES = 1024
MESH = pl.DeviceIdType.MESH
SIGN = np.int32(-(2**31))
CAP = 2048
EMPTY = 131072


def swapped(block, axis, apart):
    count = lax.axis_size(axis)
    route = []
    for low in range(count):
        high = low | 1 << apart
        if high != low and high < count:
            route += [(low, high), (high, low)]
    return lax.ppermute(block, axis, route)


def combine(first, second):
    speed_a = first[0]
    speed_b = second[0]
    best = jnp.maximum(speed_a, speed_b)
    ident = jnp.where(
        speed_a > speed_b,
        first[1],
        jnp.where(speed_b > speed_a, second[1], jnp.minimum(first[1], second[1])),
    )
    return jnp.stack([best, ident])


def dense_path(cell, vehicle, speed):
    local_best = jnp.full((CELLS,), -1.0, jnp.float32).at[cell].max(speed)
    chosen = jnp.where(speed == local_best[cell], vehicle, VEHICLES)
    local_ident = jnp.full((CELLS,), VEHICLES, jnp.int32).at[cell].min(chosen)
    paired = jnp.stack([local_best, local_ident.astype(jnp.float32)])
    outer = lax.axis_size("gx")
    inner = lax.axis_size("gy")
    nbits = (outer * inner).bit_length() - 1
    myself = lax.axis_index(("gx", "gy"))
    buffer = paired
    for level in reversed(range(nbits)):
        half = buffer.shape[1] // 2
        side = myself >> level & 1
        keep = lax.dynamic_slice_in_dim(buffer, side * half, half, 1)
        give = lax.dynamic_slice_in_dim(buffer, (1 - side) * half, half, 1)
        partner = swapped(give, ("gx", "gy"), level)
        buffer = combine(keep, partner)
    best = buffer[0]
    lowest = buffer[1].astype(jnp.int32)
    return best, jnp.where(lowest < VEHICLES, lowest, -1)


def lanes():
    return lax.broadcasted_iota(jnp.int32, (8, 128), 1)


def subs():
    return lax.broadcasted_iota(jnp.int32, (8, 128), 0)


def lane_pick(x, index):
    return jnp.take_along_axis(x, index, axis=1)


def sub_pick(x, index):
    return jnp.take_along_axis(x, index, axis=0)


def sub_bit(i):
    return ((subs() >> i) & 1) == 1


def lane_bit(i):
    return ((lanes() >> i) & 1) == 1


def total_of(counts, matrix):
    return jnp.dot(counts, matrix, preferred_element_type=jnp.float32)


def above(c1, k1, c2, k2):
    tie = c1 == c2
    return jnp.where(tie, k1, c1) > jnp.where(tie, k2, c2)


def order_pair(a, b, down):
    swap = above(*a, *b)
    if down is True:
        a, b = b, a
    elif down is not False:
        swap = swap ^ down
    low = tuple(jnp.where(swap, y, x) for x, y in zip(a, b))
    high = tuple(jnp.where(swap, x, y) for x, y in zip(a, b))
    return low, high


def order_v(x, bits, down):
    for b in bits:
        for m in range(len(x)):
            if not m >> b & 1:
                x[m], x[m | 1 << b] = order_pair(x[m], x[m | 1 << b], down(m))


def order_cross(x, pick, index, bit, down):
    other = ~bit
    for m in range(len(x)):
        d = down(m)
        wants = bit if d is False else other if d is True else bit ^ d
        c, k = x[m]
        pc, pk = pick(c, index), pick(k, index)
        swap = above(c, k, pc, pk) ^ wants
        x[m] = jnp.where(swap, pc, c), jnp.where(swap, pk, k)


def order_s(x, bits, down):
    for i in bits:
        order_cross(x, sub_pick, subs() ^ (1 << i), sub_bit(i), down)


def order_l(x, bits, down):
    for i in bits:
        order_cross(x, lane_pick, lanes() ^ (1 << i), lane_bit(i), down)


def move_pair(a, b, bit):
    mask = SIGN | np.int32(1 << bit)
    ma, mb = a[0] & mask, b[0] & mask
    a0, b0 = ma == SIGN, mb == SIGN
    a1, b1 = ma == mask, mb == mask
    low = (jnp.where(b0, b[0], jnp.where(a0, a[0], 0)), jnp.where(b0, b[1], a[1]))
    high = (jnp.where(a1, a[0], jnp.where(b1, b[0], 0)), jnp.where(a1, a[1], b[1]))
    return low, high


def move_v(x, steps):
    for bit, i in steps:
        for m in range(len(x)):
            if not m >> i & 1:
                x[m], x[m | 1 << i] = move_pair(x[m], x[m | 1 << i], 16 + bit)


def move_s(x, steps):
    for bit, i in steps:
        b = 16 + bit
        mask = SIGN | np.int32(1 << b)
        here = SIGN | (((subs() >> i) & 1) << b)
        index = subs() ^ (1 << i)
        for m in range(len(x)):
            w, k = x[m]
            pw, pk = sub_pick(w, index), sub_pick(k, index)
            stay, come = (w & mask) == here, (pw & mask) == here
            x[m] = jnp.where(come, pw, jnp.where(stay, w, 0)), jnp.where(come, pk, k)


def turned(x):
    both = []
    for w in range(2):
        t = jnp.concatenate([p[w] for p in x], axis=0).T
        both.append([t[8 * m : 8 * m + 8] for m in range(16)])
    return list(zip(*both))


def batcher(n):
    pairs = []

    def merge(lo, n, r):
        m = r * 2
        if m < n:
            merge(lo, n, m)
            merge(lo + r, n, m)
            for i in range(lo + r, lo + n - r, m):
                pairs.append((i, i + r))
        else:
            pairs.append((lo, lo + r))

    def sort(lo, n):
        if n > 1:
            m = n // 2
            sort(lo, m)
            sort(lo + m, m)
            merge(lo, n, 1)

    sort(0, n)
    return pairs


def total(x):
    s = jnp.sum(x.astype(jnp.float32), axis=0, keepdims=True)
    s = jnp.sum(s, axis=1, keepdims=True)
    return jnp.broadcast_to(s, (8, 128)).astype(jnp.int32)


def sub_prefix(x):
    before, block = jnp.zeros_like(x), x
    for i in range(3):
        other = sub_pick(block, subs() ^ (1 << i))
        before = before + jnp.where(sub_bit(i), other, 0)
        block = block + other
    return before, block


def lane_prefix(x, order):
    row = lax.broadcasted_iota(jnp.int32, (128, 128), 0)
    column = lax.broadcasted_iota(jnp.int32, (128, 128), 1)
    less = jnp.where(order(row) < order(column), 1.0, 0.0).astype(jnp.float32)
    x = x.astype(jnp.float32)
    return total_of(x, less).astype(jnp.int32), total_of(x, jnp.ones((128, 128), jnp.float32)).astype(jnp.int32)


def load(A, B, at):
    return [(A[at + m], B[at + m]) for m in range(16)]


def save(A, B, at, x):
    for m in range(16):
        A[at + m] = x[m][0]
        B[at + m] = x[m][1]


def sort_events(cell, vehicle, speed, A, B):
    flip = -(subs() & 1)
    for block in (0, 16):
        x = []
        for m in range(16):
            c = cell[block + m]
            c = (
                (c & 0x7F800)
                | ((c & 0x380) << 1)
                | ((c & 0x400) >> 3)
                | ((c & 7) << 4)
                | ((c & 0x78) >> 3)
            )
            k = (speed[block + m] * 1024.0).astype(jnp.int32) * 1024 + (1023 - vehicle[block + m])
            x.append((c ^ flip, k ^ flip))
        for i, j in batcher(16):
            x[i], x[j] = order_pair(x[i], x[j], False)
        x = [(c ^ flip, k ^ flip) for c, k in x]
        for top in (1, 2, 3):
            way = sub_bit(top) if top < 3 else block > 0
            order_s(x, reversed(range(top)), lambda m: way)
            order_v(x, (3, 2, 1, 0), lambda m: way)
        save(A, B, block, x)
    for s in range(8, 16):
        way = lane_bit(s - 8) if s < 15 else False
        if s > 10:
            for block in (0, 16):
                x = turned(load(A, B, block))
                down = lambda m: bool(m >> (s - 11) & 1)
                order_v(x, reversed(range(s - 11)), down)
                order_s(x, (2, 1, 0), down)
                save(A, B, block, turned(x))
        for m in range(16):
            pair = [(A[m], B[m]), (A[m + 16], B[m + 16])]
            if s in (9, 10):
                order_l(pair, reversed(range(s - 8)), lambda m: way)
            order_v(pair, (0,), lambda m: way)
            for h in range(2):
                A[m + 16 * h] = pair[h][0]
                B[m + 16 * h] = pair[h][1]
        for block in (0, 16):
            x = load(A, B, block)
            order_s(x, (2, 1, 0), lambda m: way)
            order_v(x, (3, 2, 1, 0), lambda m: way)
            save(A, B, block, x)


def compact_events(A, B):
    lane, sub = lanes(), subs()
    heads = [pltpu.roll(A[block], 7, 0) for block in (0, 16)]
    follows = [
        jnp.where(sub == 7, heads[1], heads[0]),
        jnp.where(sub == 7, pltpu.roll(heads[0], 127, 1), heads[1]),
    ]
    sums = []
    for block in (0, 16):
        run = jnp.zeros((8, 128), jnp.int32)
        for m in range(16):
            c = A[block + m]
            keep = c != (A[block + m + 1] if m < 15 else follows[block // 16])
            if block + m == 31:
                keep = keep | ((sub == 7) & (lane == 127))
            w = (run << 16) | (c & 0xFFFF)
            B[block + m] = B[block + m] | ((c >> 16) << 27)
            A[block + m] = jnp.where(keep, SIGN | w, 0)
            run = run + keep.astype(jnp.int32)
        sums.append(sub_prefix(run))
    ahead, every = lane_prefix(sums[0][1] + sums[1][1], lambda l: l)
    starts = [(ahead + sums[0][0]) << 16, (ahead + sums[0][1] + sums[1][0]) << 16]
    for h in range(2):
        x = load(A, B, 16 * h)
        x = [(jnp.where(w < 0, w + starts[h], 0), k) for w, k in x]
        move_v(x, [(i, i) for i in range(4)])
        move_s(x, [(4 + i, i) for i in range(3)])
        save(A, B, 16 * h, x)
    for m in range(16):
        pair = move_pair((A[m], B[m]), (A[m + 16], B[m + 16]), 16 + 7)
        for h in range(2):
            A[m + 16 * h] = pair[h][0]
            B[m + 16 * h] = pair[h][1]
    y = []
    for h in range(2):
        x = turned(load(A, B, 16 * h))
        move_s(x, [(8 + i, i) for i in range(3)])
        move_v(x, [(11 + i, i) for i in range(4)])
        y += x[:8]
    starts = group_starts([k >> 27 for _, k in y], [w < 0 for w, _ in y])
    flag = crowded(starts) | (every > 8 * CAP).astype(jnp.int32)
    y = aimed([(w, k & 0x7FFFFFF) for w, k in y], [k >> 27 for _, k in y], [w < 0 for w, _ in y], starts, 0xFFFF)
    return y, flag


def list_rank(v):
    lane = lanes()
    return (v & 7) * CAP + (subs() << 8) + ((v >> 3) << 7) + ((lane & 7) << 4) + (lane >> 3)


def group_starts(groups, valid):
    groups = [jnp.where(u, g, 8) for g, u in zip(groups, valid)]
    starts = [jnp.zeros((8, 128), jnp.int32)]
    for j in range(1, 9):
        t = jnp.zeros((8, 128), jnp.int32)
        for g in groups:
            t = t + jnp.where(g < j, 1, 0)
        starts.append(total(t))
    return starts


def crowded(starts):
    most = jnp.zeros((8, 128), jnp.int32)
    for j in range(8):
        most = jnp.maximum(most, starts[j + 1] - starts[j])
    return (most > CAP).astype(jnp.int32)


def aimed(x, groups, valid, starts, mask):
    made = []
    for v, (w, k) in enumerate(x):
        target = list_rank(v)
        moved = jnp.zeros((8, 128), jnp.int32)
        for j in range(1, 8):
            moved = jnp.where(groups[v] == j, j * CAP - starts[j], moved)
        made.append((jnp.where(valid[v], SIGN | ((target + moved) << 16) | (w & mask), 0), k))
    return made


def expand_lists(x):
    move_v(x, [(13, 2), (12, 1), (11, 0)])
    move_s(x, [(10, 2), (9, 1), (8, 0)])
    move_v(x, [(7, 3)])
    x = turned(x)
    move_s(x, [(6, 2), (5, 1), (4, 0)])
    move_v(x, [(3, 3), (2, 2), (1, 1), (0, 0)])
    return turned(x)


def pack_messages(x, out):
    for v, (w, k) in enumerate(x):
        g, h = v & 7, v >> 3
        out[g, h] = jnp.where(w < 0, w & 0xFFFF, EMPTY).astype(jnp.float32)
        out[g, 2 + h] = (k >> 10).astype(jnp.float32) * (1.0 / 1024.0)
        out[g, 4 + h] = (1023 - (k & 1023)).astype(jnp.float32)


def key_of(speed, vehicle):
    return (speed * 1024.0).astype(jnp.int32) * 1024 + (1023 - vehicle.astype(jnp.int32))


def merge_lists(inbox):
    around, back = 7 - subs(), 127 - lanes()
    x = [None] * 16
    for s in range(8):
        for h in range(2):
            pair = (inbox[s, h].astype(jnp.int32), key_of(inbox[s, 2 + h], inbox[s, 4 + h]))
            if s & 1:
                x[8 * (1 - h) + s] = tuple(lane_pick(sub_pick(w, around), back) for w in pair)
            else:
                x[8 * h + s] = pair
    for level in (1, 2, 3):
        down = (lambda m: bool(m >> level & 1)) if level < 3 else (lambda m: False)
        way = lane_bit(3 + level) if level < 3 else False
        order_v(x, reversed(range(level)), down)
        order_s(x, (2, 1, 0), down)
        order_v(x, (3,), down)
        x = turned(x)
        order_s(x, (2, 1, 0), lambda m: way)
        order_v(x, (3, 2, 1, 0), lambda m: way)
        if level < 3:
            x = turned(x)
    return x


def regroup(x):
    x = turned(x)
    groups = [c >> 13 for c, _ in x]
    valid = [c < EMPTY for c, _ in x]
    starts = group_starts(groups, valid)
    return expand_lists(aimed(x, groups, valid, starts, 0x1FFF)), crowded(starts)


def to_table(x):
    lane, sub = lanes(), subs()
    head = pltpu.roll(x[0][0], 7, 0)
    carried = jnp.where(lane < 64, pltpu.roll(head, 64, 1), pltpu.roll(head, 63, 1))
    follow = jnp.where(sub == 7, carried, head)
    run = jnp.zeros((8, 128), jnp.int32)
    y = []
    for m in range(16):
        c, k = x[m]
        keep = c != (x[m + 1][0] if m < 15 else follow)
        if m == 15:
            keep = keep | ((sub == 7) & (lane == 127))
        keep = keep & (c < EMPTY)
        y.append((jnp.where(keep, SIGN | (run << 16) | c, 0), k))
        run = run + keep.astype(jnp.int32)
    within, block = sub_prefix(run)
    ahead, _ = lane_prefix(block, lambda l: (l & 63) * 2 + (l >> 6))
    start = (within + ahead) << 16
    y = [(jnp.where(w < 0, w + start, 0), k) for w, k in y]
    move_v(y, [(i, i) for i in range(4)])
    move_s(y, [(4 + i, i) for i in range(3)])
    y = turned(y)
    move_v(y, [(7, 3)])
    move_s(y, [(8 + i, i) for i in range(3)])
    move_v(y, [(11 + i, i) for i in range(3)])
    z = []
    for q in range(4):
        for h in range(2):
            w, k = y[8 * h + q]
            z.append((jnp.where(w < 0, SIGN | ((w & 0x1FFF) << 16), 0), k))
    move_v(z, [(12, 2), (11, 1)])
    move_s(z, [(10, 2), (9, 1), (8, 0)])
    move_v(z, [(7, 0)])
    none = jnp.zeros((8, 128), jnp.int32)
    z = turned(z + [(none, none)] * 8)
    move_s(z, [(6, 2), (5, 1), (4, 0)])
    move_v(z, [(3, 3), (2, 2), (1, 1), (0, 0)])
    return turned(z)[:8]


def exchange_kernel(cell, vehicle, speed, best, ident, flags, A, B, out1, in1, out2, in2, out3, in3, mark, marks1, mark2,
                    marks2, send, recv):
    gx, gy = lax.axis_index("gx"), lax.axis_index("gy")
    y, z = gy // 8, gy % 8

    def peer(phase, j):
        if phase == 0:
            return (gx ^ j, gy)
        if phase == 1:
            return (gx, (y ^ j) * 8 + z)
        return (gx, y * 8 + (z ^ j))

    barrier = pltpu.get_barrier_semaphore()
    for phase in range(3):
        for j in range(1, 8):
            pl.semaphore_signal(barrier, inc=1, device_id=peer(phase, j), device_id_type=MESH)

    def copies(row, phase, source, target):
        return [
            pltpu.make_async_remote_copy(
                src_ref=source(j),
                dst_ref=target.at[j],
                send_sem=send.at[row, j],
                recv_sem=recv.at[row, j],
                device_id=peer(phase, j),
                device_id_type=MESH,
            )
            for j in range(1, 8)
        ]

    sort_events(cell, vehicle, speed, A, B)
    x, flag = compact_events(A, B)
    pack_messages(expand_lists(x), out1)
    pl.semaphore_wait(barrier, 21)
    first = copies(0, 0, lambda j: out1.at[gx ^ j], in1)
    for c in first:
        c.start()
    in1[0] = out1[gx]
    for c in first:
        c.wait_recv()

    x, more = regroup(merge_lists(in1))
    mark[...] = (flag | more).astype(jnp.float32)
    pack_messages(x, out2)
    second = copies(1, 1, lambda j: out2.at[y ^ j], in2)
    for c in second:
        c.start()
    flags1 = copies(2, 0, lambda j: mark, marks1)
    for c in flags1:
        c.start()
    in2[0] = out2[y]
    for c in flags1:
        c.wait_recv()
    seen = mark[...]
    for j in range(1, 8):
        seen = jnp.maximum(seen, marks1[j])
    mark2[...] = seen
    flags2 = copies(3, 1, lambda j: mark2, marks2)
    for c in flags2:
        c.start()
    for c in second:
        c.wait_recv()

    table = to_table(merge_lists(in2))
    for c in flags2:
        c.wait_recv()
    for j in range(1, 8):
        seen = jnp.maximum(seen, marks2[j])
    for v, (w, k) in enumerate(table):
        there = w < 0
        out3[v, 0] = jnp.where(there, (k >> 10).astype(jnp.float32) * (1.0 / 1024.0), -1.0)
        out3[v, 1] = jnp.where(there, (1023 - (k & 1023)).astype(jnp.float32), 1024.0) + seen * 4096.0
    third = copies(4, 2, lambda j: out3.at[z ^ j], in3)
    for c in third:
        c.start()
    in3[0] = out3[z]
    for c in third:
        c.wait_recv()
    k = key_of(in3[0, 0], in3[0, 1])
    most = in3[0, 1]
    for j in range(1, 8):
        k = jnp.maximum(k, key_of(in3[j, 0], in3[j, 1]))
        most = jnp.maximum(most, in3[j, 1])
    best[...] = jnp.where(k < 0, -1.0, (k >> 10).astype(jnp.float32) * (1.0 / 1024.0))
    ident[...] = jnp.where(k < 0, -1, 1023 - (k & 1023))
    flags[...] = most
    for group in (first, second, flags1, flags2, third):
        for c in group:
            c.wait_send()


def words(*shape):
    return pltpu.VMEM(shape + (8, 128), jnp.float32)


def sparse_path(cell, vehicle, speed):
    whole = pl.BlockSpec(memory_space=pltpu.VMEM)
    ints = lambda n: pltpu.VMEM((n, 8, 128), jnp.int32)
    return pl.pallas_call(
        exchange_kernel,
        out_shape=(
            jax.ShapeDtypeStruct((8, 128), jnp.float32),
            jax.ShapeDtypeStruct((8, 128), jnp.int32),
            jax.ShapeDtypeStruct((8, 128), jnp.float32),
        ),
        in_specs=[whole] * 3,
        out_specs=(whole,) * 3,
        scratch_shapes=[
            ints(32), ints(32),
            words(8, 6), words(8, 6), words(8, 6), words(8, 6), words(8, 2), words(8, 2),
            words(), words(8), words(), words(8),
            pltpu.SemaphoreType.DMA((5, 8)),
            pltpu.SemaphoreType.DMA((5, 8)),
        ],
        compiler_params=pltpu.CompilerParams(collective_id=0, has_side_effects=True),
    )(cell, vehicle, speed)


def per_device(cell, vehicle, speed):
    shaped = [x.reshape(32, 8, 128) for x in (cell, vehicle, speed)]
    best, ident, flags = sparse_path(*shaped)
    return lax.cond(
        flags[0, 0] > 2048.0,
        lambda: dense_path(cell, vehicle, speed),
        lambda: (best.reshape(1024), ident.reshape(1024)),
    )


def solution(mesh):
    placed = (P(("gx", "gy")), P(("gx", "gy")), P(("gx", "gy")))
    return jax.shard_map(
        per_device,
        mesh=mesh,
        in_specs=placed,
        out_specs=(P(("gx", "gy")), P(("gx", "gy"))),
        check_vma=False,
    )
```

```python
import jax
import jax.numpy as jnp
import numpy as np
from jax import lax
from jax.experimental import pallas as pl
from jax.experimental.pallas import tpu as pltpu
from jax.sharding import PartitionSpec as P

CELLS = 524288
VEHICLES = 1024
MESH = pl.DeviceIdType.MESH
SIGN = np.int32(-(2**31))
CAP = 2048
EMPTY = 131072


def swapped(block, axis, apart):
    count = lax.axis_size(axis)
    route = []
    for low in range(count):
        high = low | 1 << apart
        if high != low and high < count:
            route += [(low, high), (high, low)]
    return lax.ppermute(block, axis, route)


def combine(first, second):
    speed_a = first[0]
    speed_b = second[0]
    best = jnp.maximum(speed_a, speed_b)
    ident = jnp.where(
        speed_a > speed_b,
        first[1],
        jnp.where(speed_b > speed_a, second[1], jnp.minimum(first[1], second[1])),
    )
    return jnp.stack([best, ident])


def dense_path(cell, vehicle, speed):
    local_best = jnp.full((CELLS,), -1.0, jnp.float32).at[cell].max(speed)
    chosen = jnp.where(speed == local_best[cell], vehicle, VEHICLES)
    local_ident = jnp.full((CELLS,), VEHICLES, jnp.int32).at[cell].min(chosen)
    paired = jnp.stack([local_best, local_ident.astype(jnp.float32)])
    outer = lax.axis_size("gx")
    inner = lax.axis_size("gy")
    nbits = (outer * inner).bit_length() - 1
    myself = lax.axis_index(("gx", "gy"))
    buffer = paired
    for level in reversed(range(nbits)):
        half = buffer.shape[1] // 2
        side = myself >> level & 1
        keep = lax.dynamic_slice_in_dim(buffer, side * half, half, 1)
        give = lax.dynamic_slice_in_dim(buffer, (1 - side) * half, half, 1)
        partner = swapped(give, ("gx", "gy"), level)
        buffer = combine(keep, partner)
    best = buffer[0]
    lowest = buffer[1].astype(jnp.int32)
    return best, jnp.where(lowest < VEHICLES, lowest, -1)


def lanes():
    return lax.broadcasted_iota(jnp.int32, (8, 128), 1)


def subs():
    return lax.broadcasted_iota(jnp.int32, (8, 128), 0)


def lane_pick(x, index):
    return jnp.take_along_axis(x, index, axis=1)


def sub_pick(x, index):
    return jnp.take_along_axis(x, index, axis=0)


def sub_bit(i):
    return ((subs() >> i) & 1) == 1


def lane_bit(i):
    return ((lanes() >> i) & 1) == 1


def total_of(counts, matrix):
    return jnp.dot(counts, matrix, preferred_element_type=jnp.float32)


def above(c1, k1, c2, k2):
    tie = c1 == c2
    return jnp.where(tie, k1, c1) > jnp.where(tie, k2, c2)


def order_pair(a, b, down):
    swap = above(*a, *b)
    if down is True:
        a, b = b, a
    elif down is not False:
        swap = swap ^ down
    low = tuple(jnp.where(swap, y, x) for x, y in zip(a, b))
    high = tuple(jnp.where(swap, x, y) for x, y in zip(a, b))
    return low, high


def order_v(x, bits, down):
    for b in bits:
        for m in range(len(x)):
            if not m >> b & 1:
                x[m], x[m | 1 << b] = order_pair(x[m], x[m | 1 << b], down(m))


def order_cross(x, pick, index, bit, down):
    other = ~bit
    for m in range(len(x)):
        d = down(m)
        wants = bit if d is False else other if d is True else bit ^ d
        c, k = x[m]
        pc, pk = pick(c, index), pick(k, index)
        swap = above(c, k, pc, pk) ^ wants
        x[m] = jnp.where(swap, pc, c), jnp.where(swap, pk, k)


def order_s(x, bits, down):
    for i in bits:
        order_cross(x, sub_pick, subs() ^ (1 << i), sub_bit(i), down)


def order_l(x, bits, down):
    for i in bits:
        order_cross(x, lane_pick, lanes() ^ (1 << i), lane_bit(i), down)


def move_pair(a, b, bit):
    mask = SIGN | np.int32(1 << bit)
    ma, mb = a[0] & mask, b[0] & mask
    a0, b0 = ma == SIGN, mb == SIGN
    a1, b1 = ma == mask, mb == mask
    low = (jnp.where(b0, b[0], jnp.where(a0, a[0], 0)), jnp.where(b0, b[1], a[1]))
    high = (jnp.where(a1, a[0], jnp.where(b1, b[0], 0)), jnp.where(a1, a[1], b[1]))
    return low, high


def move_v(x, steps):
    for bit, i in steps:
        for m in range(len(x)):
            if not m >> i & 1:
                x[m], x[m | 1 << i] = move_pair(x[m], x[m | 1 << i], 16 + bit)


def move_s(x, steps):
    for bit, i in steps:
        b = 16 + bit
        mask = SIGN | np.int32(1 << b)
        here = SIGN | (((subs() >> i) & 1) << b)
        index = subs() ^ (1 << i)
        for m in range(len(x)):
            w, k = x[m]
            pw, pk = sub_pick(w, index), sub_pick(k, index)
            stay, come = (w & mask) == here, (pw & mask) == here
            x[m] = jnp.where(come, pw, jnp.where(stay, w, 0)), jnp.where(come, pk, k)


def turned(x):
    both = []
    for w in range(2):
        t = jnp.concatenate([p[w] for p in x], axis=0).T
        both.append([t[8 * m : 8 * m + 8] for m in range(16)])
    return list(zip(*both))


def batcher(n):
    pairs = []

    def merge(lo, n, r):
        m = r * 2
        if m < n:
            merge(lo, n, m)
            merge(lo + r, n, m)
            for i in range(lo + r, lo + n - r, m):
                pairs.append((i, i + r))
        else:
            pairs.append((lo, lo + r))

    def sort(lo, n):
        if n > 1:
            m = n // 2
            sort(lo, m)
            sort(lo + m, m)
            merge(lo, n, 1)

    sort(0, n)
    return pairs


def total(x):
    s = jnp.sum(x.astype(jnp.float32), axis=0, keepdims=True)
    s = jnp.sum(s, axis=1, keepdims=True)
    return jnp.broadcast_to(s, (8, 128)).astype(jnp.int32)


def sub_prefix(x):
    before, block = jnp.zeros_like(x), x
    for i in range(3):
        other = sub_pick(block, subs() ^ (1 << i))
        before = before + jnp.where(sub_bit(i), other, 0)
        block = block + other
    return before, block


def lane_prefix(x, order):
    row = lax.broadcasted_iota(jnp.int32, (128, 128), 0)
    column = lax.broadcasted_iota(jnp.int32, (128, 128), 1)
    less = jnp.where(order(row) < order(column), 1.0, 0.0).astype(jnp.float32)
    x = x.astype(jnp.float32)
    return total_of(x, less).astype(jnp.int32), total_of(x, jnp.ones((128, 128), jnp.float32)).astype(jnp.int32)


def load(A, B, at):
    return [(A[at + m], B[at + m]) for m in range(16)]


def save(A, B, at, x):
    for m in range(16):
        A[at + m] = x[m][0]
        B[at + m] = x[m][1]


def sort_events(cell, vehicle, speed, A, B):
    flip = -(subs() & 1)
    for block in (0, 16):
        x = []
        for m in range(16):
            c = cell[block + m]
            c = (
                (c & 0x7F800)
                | ((c & 0x380) << 1)
                | ((c & 0x400) >> 3)
                | ((c & 7) << 4)
                | ((c & 0x78) >> 3)
            )
            k = (speed[block + m] * 1024.0).astype(jnp.int32) * 1024 + (1023 - vehicle[block + m])
            x.append((c ^ flip, k ^ flip))
        for i, j in batcher(16):
            x[i], x[j] = order_pair(x[i], x[j], False)
        x = [(c ^ flip, k ^ flip) for c, k in x]
        for top in (1, 2, 3):
            way = sub_bit(top) if top < 3 else block > 0
            order_s(x, reversed(range(top)), lambda m: way)
            order_v(x, (3, 2, 1, 0), lambda m: way)
        save(A, B, block, x)
    for s in range(8, 16):
        way = lane_bit(s - 8) if s < 15 else False
        if s > 10:
            for block in (0, 16):
                x = turned(load(A, B, block))
                down = lambda m: bool(m >> (s - 11) & 1)
                order_v(x, reversed(range(s - 11)), down)
                order_s(x, (2, 1, 0), down)
                save(A, B, block, turned(x))
        for m in range(16):
            pair = [(A[m], B[m]), (A[m + 16], B[m + 16])]
            if s in (9, 10):
                order_l(pair, reversed(range(s - 8)), lambda m: way)
            order_v(pair, (0,), lambda m: way)
            for h in range(2):
                A[m + 16 * h] = pair[h][0]
                B[m + 16 * h] = pair[h][1]
        for block in (0, 16):
            x = load(A, B, block)
            order_s(x, (2, 1, 0), lambda m: way)
            order_v(x, (3, 2, 1, 0), lambda m: way)
            save(A, B, block, x)


def compact_events(A, B):
    lane, sub = lanes(), subs()
    heads = [pltpu.roll(A[block], 7, 0) for block in (0, 16)]
    follows = [
        jnp.where(sub == 7, heads[1], heads[0]),
        jnp.where(sub == 7, pltpu.roll(heads[0], 127, 1), heads[1]),
    ]
    sums = []
    for block in (0, 16):
        run = jnp.zeros((8, 128), jnp.int32)
        for m in range(16):
            c = A[block + m]
            keep = c != (A[block + m + 1] if m < 15 else follows[block // 16])
            if block + m == 31:
                keep = keep | ((sub == 7) & (lane == 127))
            w = (run << 16) | (c & 0xFFFF)
            B[block + m] = B[block + m] | ((c >> 16) << 27)
            A[block + m] = jnp.where(keep, SIGN | w, 0)
            run = run + keep.astype(jnp.int32)
        sums.append(sub_prefix(run))
    ahead, every = lane_prefix(sums[0][1] + sums[1][1], lambda l: l)
    starts = [(ahead + sums[0][0]) << 16, (ahead + sums[0][1] + sums[1][0]) << 16]
    for h in range(2):
        x = load(A, B, 16 * h)
        x = [(jnp.where(w < 0, w + starts[h], 0), k) for w, k in x]
        move_v(x, [(i, i) for i in range(4)])
        move_s(x, [(4 + i, i) for i in range(3)])
        save(A, B, 16 * h, x)
    for m in range(16):
        pair = move_pair((A[m], B[m]), (A[m + 16], B[m + 16]), 16 + 7)
        for h in range(2):
            A[m + 16 * h] = pair[h][0]
            B[m + 16 * h] = pair[h][1]
    y = []
    for h in range(2):
        x = turned(load(A, B, 16 * h))
        move_s(x, [(8 + i, i) for i in range(3)])
        move_v(x, [(11 + i, i) for i in range(4)])
        y += x[:8]
    starts = group_starts([k >> 27 for _, k in y], [w < 0 for w, _ in y])
    flag = crowded(starts) | (every > 8 * CAP).astype(jnp.int32)
    y = aimed([(w, k & 0x7FFFFFF) for w, k in y], [k >> 27 for _, k in y], [w < 0 for w, _ in y], starts, 0xFFFF)
    return y, flag


def list_rank(v):
    lane = lanes()
    return (v & 7) * CAP + (subs() << 8) + ((v >> 3) << 7) + ((lane & 7) << 4) + (lane >> 3)


def group_starts(groups, valid):
    groups = [jnp.where(u, g, 8) for g, u in zip(groups, valid)]
    starts = [jnp.zeros((8, 128), jnp.int32)]
    for j in range(1, 9):
        t = jnp.zeros((8, 128), jnp.int32)
        for g in groups:
            t = t + jnp.where(g < j, 1, 0)
        starts.append(total(t))
    return starts


def crowded(starts):
    most = jnp.zeros((8, 128), jnp.int32)
    for j in range(8):
        most = jnp.maximum(most, starts[j + 1] - starts[j])
    return (most > CAP).astype(jnp.int32)


def aimed(x, groups, valid, starts, mask):
    made = []
    for v, (w, k) in enumerate(x):
        target = list_rank(v)
        moved = jnp.zeros((8, 128), jnp.int32)
        for j in range(1, 8):
            moved = jnp.where(groups[v] == j, j * CAP - starts[j], moved)
        made.append((jnp.where(valid[v], SIGN | ((target + moved) << 16) | (w & mask), 0), k))
    return made


def expand_lists(x):
    move_v(x, [(13, 2), (12, 1), (11, 0)])
    move_s(x, [(10, 2), (9, 1), (8, 0)])
    move_v(x, [(7, 3)])
    x = turned(x)
    move_s(x, [(6, 2), (5, 1), (4, 0)])
    move_v(x, [(3, 3), (2, 2), (1, 1), (0, 0)])
    return turned(x)


def pack_messages(x, out):
    for v, (w, k) in enumerate(x):
        g, h = v & 7, v >> 3
        out[g, h] = jnp.where(w < 0, w & 0xFFFF, EMPTY).astype(jnp.float32)
        out[g, 2 + h] = (k >> 10).astype(jnp.float32) * (1.0 / 1024.0)
        out[g, 4 + h] = (1023 - (k & 1023)).astype(jnp.float32)


def key_of(speed, vehicle):
    return (speed * 1024.0).astype(jnp.int32) * 1024 + (1023 - vehicle.astype(jnp.int32))


def merge_lists(inbox):
    around, back = 7 - subs(), 127 - lanes()
    x = [None] * 16
    for s in range(8):
        for h in range(2):
            pair = (inbox[s, h].astype(jnp.int32), key_of(inbox[s, 2 + h], inbox[s, 4 + h]))
            if s & 1:
                x[8 * (1 - h) + s] = tuple(lane_pick(sub_pick(w, around), back) for w in pair)
            else:
                x[8 * h + s] = pair
    for level in (1, 2, 3):
        down = (lambda m: bool(m >> level & 1)) if level < 3 else (lambda m: False)
        way = lane_bit(3 + level) if level < 3 else False
        order_v(x, reversed(range(level)), down)
        order_s(x, (2, 1, 0), down)
        order_v(x, (3,), down)
        x = turned(x)
        order_s(x, (2, 1, 0), lambda m: way)
        order_v(x, (3, 2, 1, 0), lambda m: way)
        if level < 3:
            x = turned(x)
    return x


def best_of_cells(x):
    lane, sub = lanes(), subs()
    head = pltpu.roll(x[0][0], 7, 0)
    carried = jnp.where(lane < 64, pltpu.roll(head, 64, 1), pltpu.roll(head, 63, 1))
    follow = jnp.where(sub == 7, carried, head)
    run = jnp.zeros((8, 128), jnp.int32)
    y = []
    for m in range(16):
        c, k = x[m]
        keep = c != (x[m + 1][0] if m < 15 else follow)
        if m == 15:
            keep = keep | ((sub == 7) & (lane == 127))
        keep = keep & (c < EMPTY)
        y.append((jnp.where(keep, SIGN | (run << 16) | c, 0), k))
        run = run + keep.astype(jnp.int32)
    within, block = sub_prefix(run)
    ahead, _ = lane_prefix(block, lambda l: (l & 63) * 2 + (l >> 6))
    start = (within + ahead) << 16
    y = [(jnp.where(w < 0, w + start, 0), k) for w, k in y]
    move_v(y, [(i, i) for i in range(4)])
    move_s(y, [(4 + i, i) for i in range(3)])
    y = turned(y)
    move_v(y, [(7, 3)])
    move_s(y, [(8 + i, i) for i in range(3)])
    move_v(y, [(11 + i, i) for i in range(3)])
    return y


def regroup(x):
    y = best_of_cells(x)
    groups = [(w >> 13) & 7 for w, _ in y]
    valid = [w < 0 for w, _ in y]
    starts = group_starts(groups, valid)
    return expand_lists(aimed(y, groups, valid, starts, 0x1FFF)), crowded(starts)


def to_table(x):
    y = best_of_cells(x)
    z = []
    for q in range(4):
        for h in range(2):
            w, k = y[8 * h + q]
            z.append((jnp.where(w < 0, SIGN | ((w & 0x1FFF) << 16), 0), k))
    move_v(z, [(12, 2), (11, 1)])
    move_s(z, [(10, 2), (9, 1), (8, 0)])
    move_v(z, [(7, 0)])
    none = jnp.zeros((8, 128), jnp.int32)
    z = turned(z + [(none, none)] * 8)
    move_s(z, [(6, 2), (5, 1), (4, 0)])
    move_v(z, [(3, 3), (2, 2), (1, 1), (0, 0)])
    return turned(z)[:8]


def exchange_kernel(cell, vehicle, speed, best, ident, flags, A, B, out1, in1, out2, in2, out3, in3, mark, marks1, mark2,
                    marks2, send, recv):
    gx, gy = lax.axis_index("gx"), lax.axis_index("gy")
    y, z = gy // 8, gy % 8

    def peer(phase, j):
        if phase == 0:
            return (gx ^ j, gy)
        if phase == 1:
            return (gx, (y ^ j) * 8 + z)
        return (gx, y * 8 + (z ^ j))

    barrier = pltpu.get_barrier_semaphore()
    for phase in range(3):
        for j in range(1, 8):
            pl.semaphore_signal(barrier, inc=1, device_id=peer(phase, j), device_id_type=MESH)

    def copies(row, phase, source, target):
        return [
            pltpu.make_async_remote_copy(
                src_ref=source(j),
                dst_ref=target.at[j],
                send_sem=send.at[row, j],
                recv_sem=recv.at[row, j],
                device_id=peer(phase, j),
                device_id_type=MESH,
            )
            for j in range(1, 8)
        ]

    sort_events(cell, vehicle, speed, A, B)
    x, flag = compact_events(A, B)
    pack_messages(expand_lists(x), out1)
    pl.semaphore_wait(barrier, 21)
    first = copies(0, 0, lambda j: out1.at[gx ^ j], in1)
    for c in first:
        c.start()
    in1[0] = out1[gx]
    for c in first:
        c.wait_recv()

    x, more = regroup(merge_lists(in1))
    mark[...] = (flag | more).astype(jnp.float32)
    pack_messages(x, out2)
    second = copies(1, 1, lambda j: out2.at[y ^ j], in2)
    for c in second:
        c.start()
    flags1 = copies(2, 0, lambda j: mark, marks1)
    for c in flags1:
        c.start()
    in2[0] = out2[y]
    for c in flags1:
        c.wait_recv()
    seen = mark[...]
    for j in range(1, 8):
        seen = jnp.maximum(seen, marks1[j])
    mark2[...] = seen
    flags2 = copies(3, 1, lambda j: mark2, marks2)
    for c in flags2:
        c.start()
    for c in second:
        c.wait_recv()

    table = to_table(merge_lists(in2))
    for c in flags2:
        c.wait_recv()
    for j in range(1, 8):
        seen = jnp.maximum(seen, marks2[j])
    for v, (w, k) in enumerate(table):
        there = w < 0
        out3[v, 0] = jnp.where(there, (k >> 10).astype(jnp.float32) * (1.0 / 1024.0), -1.0)
        out3[v, 1] = jnp.where(there, (1023 - (k & 1023)).astype(jnp.float32), 1024.0) + seen * 4096.0
    third = copies(4, 2, lambda j: out3.at[z ^ j], in3)
    for c in third:
        c.start()
    in3[0] = out3[z]
    for c in third:
        c.wait_recv()
    k = key_of(in3[0, 0], in3[0, 1])
    most = in3[0, 1]
    for j in range(1, 8):
        k = jnp.maximum(k, key_of(in3[j, 0], in3[j, 1]))
        most = jnp.maximum(most, in3[j, 1])
    best[...] = jnp.where(k < 0, -1.0, (k >> 10).astype(jnp.float32) * (1.0 / 1024.0))
    ident[...] = jnp.where(k < 0, -1, 1023 - (k & 1023))
    flags[0, 0] = jnp.max(most).astype(jnp.int32)
    for group in (first, second, flags1, flags2, third):
        for c in group:
            c.wait_send()


def words(*shape):
    return pltpu.VMEM(shape + (8, 128), jnp.float32)


def sparse_path(cell, vehicle, speed):
    whole = pl.BlockSpec(memory_space=pltpu.VMEM)
    ints = lambda n: pltpu.VMEM((n, 8, 128), jnp.int32)
    return pl.pallas_call(
        exchange_kernel,
        out_shape=(
            jax.ShapeDtypeStruct((8, 128), jnp.float32),
            jax.ShapeDtypeStruct((8, 128), jnp.int32),
            jax.ShapeDtypeStruct((1, 1), jnp.int32),
        ),
        in_specs=[whole] * 3,
        out_specs=(whole, whole, pl.BlockSpec(memory_space=pltpu.SMEM)),
        scratch_shapes=[
            ints(32), ints(32),
            words(8, 6), words(8, 6), words(8, 6), words(8, 6), words(8, 2), words(8, 2),
            words(), words(8), words(), words(8),
            pltpu.SemaphoreType.DMA((5, 8)),
            pltpu.SemaphoreType.DMA((5, 8)),
        ],
        compiler_params=pltpu.CompilerParams(collective_id=0, has_side_effects=True),
    )(cell, vehicle, speed)


def per_device(cell, vehicle, speed):
    shaped = [x.reshape(32, 8, 128) for x in (cell, vehicle, speed)]
    best, ident, flags = sparse_path(*shaped)
    return lax.cond(
        flags[0, 0] > 2048,
        lambda: dense_path(cell, vehicle, speed),
        lambda: (best.reshape(1024), ident.reshape(1024)),
    )


def solution(mesh):
    placed = (P(("gx", "gy")), P(("gx", "gy")), P(("gx", "gy")))
    return jax.shard_map(
        per_device,
        mesh=mesh,
        in_specs=placed,
        out_specs=(P(("gx", "gy")), P(("gx", "gy"))),
        check_vma=False,
    )
```

```python
import jax
import jax.numpy as jnp
import numpy as np
from jax import lax
from jax.experimental import pallas as pl
from jax.experimental.pallas import tpu as pltpu
from jax.sharding import PartitionSpec as P

CELLS = 524288
VEHICLES = 1024
MESH = pl.DeviceIdType.MESH
SIGN = np.int32(-(2**31))
CAP = 2048
SHORT = 1536
EMPTY = 131072


def swapped(block, axis, apart):
    count = lax.axis_size(axis)
    route = []
    for low in range(count):
        high = low | 1 << apart
        if high != low and high < count:
            route += [(low, high), (high, low)]
    return lax.ppermute(block, axis, route)


def combine(first, second):
    speed_a = first[0]
    speed_b = second[0]
    best = jnp.maximum(speed_a, speed_b)
    ident = jnp.where(
        speed_a > speed_b,
        first[1],
        jnp.where(speed_b > speed_a, second[1], jnp.minimum(first[1], second[1])),
    )
    return jnp.stack([best, ident])


def dense_path(cell, vehicle, speed):
    local_best = jnp.full((CELLS,), -1.0, jnp.float32).at[cell].max(speed)
    chosen = jnp.where(speed == local_best[cell], vehicle, VEHICLES)
    local_ident = jnp.full((CELLS,), VEHICLES, jnp.int32).at[cell].min(chosen)
    paired = jnp.stack([local_best, local_ident.astype(jnp.float32)])
    outer = lax.axis_size("gx")
    inner = lax.axis_size("gy")
    nbits = (outer * inner).bit_length() - 1
    myself = lax.axis_index(("gx", "gy"))
    buffer = paired
    for level in reversed(range(nbits)):
        half = buffer.shape[1] // 2
        side = myself >> level & 1
        keep = lax.dynamic_slice_in_dim(buffer, side * half, half, 1)
        give = lax.dynamic_slice_in_dim(buffer, (1 - side) * half, half, 1)
        partner = swapped(give, ("gx", "gy"), level)
        buffer = combine(keep, partner)
    best = buffer[0]
    lowest = buffer[1].astype(jnp.int32)
    top_vehicle = jnp.where(lowest < VEHICLES, lowest, -1)
    return jnp.stack([best, top_vehicle.astype(jnp.float32)]).reshape(2, 8, 128)


def lanes():
    return lax.broadcasted_iota(jnp.int32, (8, 128), 1)


def subs():
    return lax.broadcasted_iota(jnp.int32, (8, 128), 0)


def lane_pick(x, index):
    return jnp.take_along_axis(x, index, axis=1)


def sub_pick(x, index):
    return jnp.take_along_axis(x, index, axis=0)


def sub_bit(i):
    return ((subs() >> i) & 1) == 1


def lane_bit(i):
    return ((lanes() >> i) & 1) == 1


def total_of(counts, matrix):
    return jnp.dot(counts, matrix, preferred_element_type=jnp.float32)


def above(c1, k1, c2, k2):
    tie = c1 == c2
    return jnp.where(tie, k1, c1) > jnp.where(tie, k2, c2)


def order_pair(a, b, down):
    swap = above(*a, *b)
    if down is True:
        a, b = b, a
    elif down is not False:
        swap = swap ^ down
    low = tuple(jnp.where(swap, y, x) for x, y in zip(a, b))
    high = tuple(jnp.where(swap, x, y) for x, y in zip(a, b))
    return low, high


def order_v(x, bits, down):
    for b in bits:
        for m in range(len(x)):
            if not m >> b & 1:
                x[m], x[m | 1 << b] = order_pair(x[m], x[m | 1 << b], down(m))


def order_cross(x, pick, index, bit, down):
    other = ~bit
    for m in range(len(x)):
        d = down(m)
        wants = bit if d is False else other if d is True else bit ^ d
        c, k = x[m]
        pc, pk = pick(c, index), pick(k, index)
        swap = above(c, k, pc, pk) ^ wants
        x[m] = jnp.where(swap, pc, c), jnp.where(swap, pk, k)


def order_s(x, bits, down):
    for i in bits:
        order_cross(x, sub_pick, subs() ^ (1 << i), sub_bit(i), down)


def order_l(x, bits, down):
    for i in bits:
        order_cross(x, lane_pick, lanes() ^ (1 << i), lane_bit(i), down)


def move_pair(a, b, bit):
    mask = SIGN | np.int32(1 << bit)
    ma, mb = a[0] & mask, b[0] & mask
    a0, b0 = ma == SIGN, mb == SIGN
    a1, b1 = ma == mask, mb == mask
    low = (jnp.where(b0, b[0], jnp.where(a0, a[0], 0)), jnp.where(b0, b[1], a[1]))
    high = (jnp.where(a1, a[0], jnp.where(b1, b[0], 0)), jnp.where(a1, a[1], b[1]))
    return low, high


def move_v(x, steps):
    for bit, i in steps:
        for m in range(len(x)):
            if not m >> i & 1:
                x[m], x[m | 1 << i] = move_pair(x[m], x[m | 1 << i], 16 + bit)


def move_s(x, steps):
    for bit, i in steps:
        b = 16 + bit
        mask = SIGN | np.int32(1 << b)
        here = SIGN | (((subs() >> i) & 1) << b)
        index = subs() ^ (1 << i)
        for m in range(len(x)):
            w, k = x[m]
            pw, pk = sub_pick(w, index), sub_pick(k, index)
            stay, come = (w & mask) == here, (pw & mask) == here
            x[m] = jnp.where(come, pw, jnp.where(stay, w, 0)), jnp.where(come, pk, k)


def turned(x):
    both = []
    for w in range(2):
        t = jnp.concatenate([p[w] for p in x], axis=0).T
        both.append([t[8 * m : 8 * m + 8] for m in range(16)])
    return list(zip(*both))


def batcher(n):
    pairs = []

    def merge(lo, n, r):
        m = r * 2
        if m < n:
            merge(lo, n, m)
            merge(lo + r, n, m)
            for i in range(lo + r, lo + n - r, m):
                pairs.append((i, i + r))
        else:
            pairs.append((lo, lo + r))

    def sort(lo, n):
        if n > 1:
            m = n // 2
            sort(lo, m)
            sort(lo + m, m)
            merge(lo, n, 1)

    sort(0, n)
    return pairs


def total(x):
    s = jnp.sum(x.astype(jnp.float32), axis=0, keepdims=True)
    s = jnp.sum(s, axis=1, keepdims=True)
    return jnp.broadcast_to(s, (8, 128)).astype(jnp.int32)


def sub_prefix(x):
    before, block = jnp.zeros_like(x), x
    for i in range(3):
        other = sub_pick(block, subs() ^ (1 << i))
        before = before + jnp.where(sub_bit(i), other, 0)
        block = block + other
    return before, block


def lane_prefix(x, order, places):
    row = lax.broadcasted_iota(jnp.int32, (128, 128), 0)
    column = lax.broadcasted_iota(jnp.int32, (128, 128), 1)
    x = x.astype(jnp.float32)
    before = [jnp.where(order(row) < place(column), 1.0, 0.0).astype(jnp.float32) for place in places]
    return [total_of(x, m).astype(jnp.int32) for m in before + [jnp.ones((128, 128), jnp.float32)]]


def load(A, B, at):
    return [(A[at + m], B[at + m]) for m in range(16)]


def save(A, B, at, x):
    for m in range(16):
        A[at + m] = x[m][0]
        B[at + m] = x[m][1]


def sort_events(cell, vehicle, speed, A, B):
    flip = -(subs() & 1)
    for block in (0, 16):
        x = []
        for m in range(16):
            c = cell[block + m]
            c = (c & 0x7FF80) | ((c & 7) << 4) | ((c >> 3) & 15)
            k = (speed[block + m] * 1024.0).astype(jnp.int32) * 1024 + (1023 - vehicle[block + m])
            x.append((c ^ flip, k ^ flip))
        for i, j in batcher(16):
            x[i], x[j] = order_pair(x[i], x[j], False)
        x = [(c ^ flip, k ^ flip) for c, k in x]
        for top in (1, 2, 3):
            way = sub_bit(top) if top < 3 else lane_bit(0)
            order_s(x, reversed(range(top)), lambda m: way)
            order_v(x, (3, 2, 1, 0), lambda m: way)
        save(A, B, block, x)
    for s in range(8, 16):
        if s > 10:
            for block in (0, 16):
                x = turned(load(A, B, block))
                order_v(x, reversed(range(s - 11)), lambda m: bool(m >> (s - 11) & 1))
                save(A, B, block, x)
            for m in range(16):
                pair = [(A[m], B[m]), (A[m + 16], B[m + 16])]
                order_v(pair, (0,), lambda _: bool(m >> (s - 11) & 1))
                for h in range(2):
                    A[m + 16 * h] = pair[h][0]
                    B[m + 16 * h] = pair[h][1]
        for block in (0, 16):
            x = load(A, B, block)
            way = lane_bit(s - 7) if s < 10 else block > 0 if s == 10 else lane_bit(s - 8) if s < 15 else False
            if s > 9:
                x = turned(x) if s == 10 else x
                order_s(x, (2, 1, 0), lambda m: way if s == 10 else bool(m >> (s - 11) & 1))
                x = turned(x)
            else:
                order_l(x, reversed(range(s - 7)), lambda m: way)
            order_s(x, (2, 1, 0), lambda m: way)
            order_v(x, (3, 2, 1, 0), lambda m: way)
            save(A, B, block, x)


def compact_events(A, B):
    lane, sub = lanes(), subs()
    heads = [pltpu.roll(A[block], 7, 0) for block in (0, 16)]
    nexts = [pltpu.roll(x, 127, 1) for x in heads]
    edge = (lane & 7) == 7
    follows = [
        jnp.where(sub == 7, jnp.where(edge, pltpu.roll(heads[1], 7, 1), nexts[0]), heads[0]),
        jnp.where(sub == 7, jnp.where(edge, nexts[0], nexts[1]), heads[1]),
    ]
    sums = []
    for block in (0, 16):
        run = jnp.zeros((8, 128), jnp.int32)
        for m in range(16):
            c = A[block + m]
            keep = c != (A[block + m + 1] if m < 15 else follows[block // 16])
            if block + m == 31:
                keep = keep | ((sub == 7) & (lane == 127))
            w = (run << 16) | (c & 0xFFFF)
            B[block + m] = B[block + m] | ((c >> 16) << 27)
            A[block + m] = jnp.where(keep, SIGN | w, 0)
            run = run + keep.astype(jnp.int32)
        sums.append(sub_prefix(run))
    orders = [lambda l: ((l >> 3) << 4) + (l & 7), lambda l: ((l >> 3) << 4) + (l & 7) + 8]
    parts = [lane_prefix(sums[h][1], orders[h], orders) for h in range(2)]
    every = parts[0][2] + parts[1][2]
    for h in range(2):
        start = (parts[0][h] + parts[1][h] + sums[h][0]) << 16
        x = [(jnp.where(w < 0, w + start, 0), k) for w, k in load(A, B, 16 * h)]
        move_v(x, [(i, i) for i in range(4)])
        move_s(x, [(4 + i, i) for i in range(3)])
        x = turned(x)
        move_s(x, [(7 + i, i) for i in range(3)])
        save(A, B, 16 * h, x)
    for m in range(16):
        pair = move_pair((A[m], B[m]), (A[m + 16], B[m + 16]), 16 + 10)
        for h in range(2):
            A[m + 16 * h] = pair[h][0]
            B[m + 16 * h] = pair[h][1]
    y = []
    for h in range(2):
        x = load(A, B, 16 * h)
        move_v(x, [(11 + i, i) for i in range(4)])
        y += x[:8]
    starts = group_starts([k >> 27 for _, k in y], [w < 0 for w, _ in y])
    flag = crowded(starts, CAP) | (every > 8 * CAP).astype(jnp.int32)
    y = aimed([(w, k & 0x7FFFFFF) for w, k in y], [k >> 27 for _, k in y], [w < 0 for w, _ in y], starts, 0xFFFF)
    return y, flag


def list_rank(v):
    lane = lanes()
    return (v & 7) * CAP + ((v >> 3) << 10) + (subs() << 7) + ((lane & 7) << 4) + (lane >> 3)


def group_starts(groups, valid):
    groups = [jnp.where(u, g, 8) for g, u in zip(groups, valid)]
    starts = [jnp.zeros((8, 128), jnp.int32)]
    for j in range(1, 9):
        t = jnp.zeros((8, 128), jnp.int32)
        for g in groups:
            t = t + jnp.where(g < j, 1, 0)
        starts.append(total(t))
    return starts


def crowded(starts, room):
    most = jnp.zeros((8, 128), jnp.int32)
    for j in range(8):
        most = jnp.maximum(most, starts[j + 1] - starts[j])
    return (most > room).astype(jnp.int32)


def aimed(x, groups, valid, starts, mask):
    made = []
    for v, (w, k) in enumerate(x):
        target = list_rank(v)
        moved = jnp.zeros((8, 128), jnp.int32)
        for j in range(1, 8):
            moved = jnp.where(groups[v] == j, j * CAP - starts[j], moved)
        made.append((jnp.where(valid[v], SIGN | ((target + moved) << 16) | (w & mask), 0), k))
    return made


def expand_lists(x):
    move_v(x, [(13, 2), (12, 1), (11, 0), (10, 3)])
    move_s(x, [(9, 2), (8, 1), (7, 0)])
    x = turned(x)
    move_s(x, [(6, 2), (5, 1), (4, 0)])
    move_v(x, [(3, 3), (2, 2), (1, 1), (0, 0)])
    return turned(x)


def planes(w, k):
    return (
        jnp.where(w < 0, w & 0xFFFF, EMPTY).astype(jnp.float32),
        (k >> 10).astype(jnp.float32) * (1.0 / 1024.0),
        (1023 - (k & 1023)).astype(jnp.float32),
    )


def pack_messages(x, out):
    for v, pair in enumerate(x):
        for p, plane in enumerate(planes(*pair)):
            out[v & 7, 2 * p + (v >> 3)] = plane


def pack_short(x, out):
    for v, pair in enumerate(x):
        for p, plane in enumerate(planes(*pair)):
            if v < 8:
                out[v, 3 * p] = plane[:4]
                out[v, 3 * p + 1] = plane[4:]
            else:
                out[v - 8, 3 * p + 2] = plane[:4]


def key_of(speed, vehicle):
    return (speed * 1024.0).astype(jnp.int32) * 1024 + (1023 - vehicle.astype(jnp.int32))


def merge_lists(inbox):
    around, back = 7 - subs(), 127 - lanes()
    x = [None] * 16
    for s in range(8):
        for h in range(2):
            pair = (inbox[s, h].astype(jnp.int32), key_of(inbox[s, 2 + h], inbox[s, 4 + h]))
            if s & 1:
                x[8 * (1 - h) + s] = tuple(lane_pick(sub_pick(w, around), back) for w in pair)
            else:
                x[8 * h + s] = pair
    for level in (1, 2, 3):
        down = (lambda m: bool(m >> level & 1)) if level < 3 else (lambda m: False)
        way = lane_bit(3 + level) if level < 3 else False
        order_v(x, (*reversed(range(level)), 3), down)
        order_s(x, (2, 1, 0), down)
        x = turned(x)
        order_s(x, (2, 1, 0), lambda m: way)
        order_v(x, (3, 2, 1, 0), lambda m: way)
        if level < 3:
            x = turned(x)
    return x


def best_of_cells(x):
    lane, sub = lanes(), subs()
    head = pltpu.roll(x[0][0], 7, 0)
    beyond = jnp.where(lane < 64, pltpu.roll(head, 71, 1), pltpu.roll(head, 63, 1))
    carried = jnp.where((lane & 7) == 7, beyond, pltpu.roll(head, 127, 1))
    follow = jnp.where(sub == 7, carried, head)
    run = jnp.zeros((8, 128), jnp.int32)
    y = []
    for m in range(16):
        c, k = x[m]
        keep = c != (x[m + 1][0] if m < 15 else follow)
        if m == 15:
            keep = keep | ((sub == 7) & (lane == 127))
        keep = keep & (c < EMPTY)
        y.append((jnp.where(keep, SIGN | (run << 16) | c, 0), k))
        run = run + keep.astype(jnp.int32)
    within, block = sub_prefix(run)
    order = lambda l: (((l >> 3) & 7) << 4) + ((l >> 6) << 3) + (l & 7)
    ahead = lane_prefix(block, order, [order])[0]
    start = (within + ahead) << 16
    y = [(jnp.where(w < 0, w + start, 0), k) for w, k in y]
    move_v(y, [(i, i) for i in range(4)])
    move_s(y, [(4 + i, i) for i in range(3)])
    y = turned(y)
    move_s(y, [(7 + i, i) for i in range(3)])
    move_v(y, [(10, 3), (11, 0), (12, 1), (13, 2)])
    return y


def regroup(x):
    y = best_of_cells(x)
    groups = [(w >> 13) & 7 for w, _ in y]
    valid = [w < 0 for w, _ in y]
    starts = group_starts(groups, valid)
    return expand_lists(aimed(y, groups, valid, starts, 0x1FFF)), crowded(starts, SHORT)


def short_list(inbox, s):
    made = []
    for h in range(2):
        low, high = (3 * h, 1) if h == 0 else (2, 2)
        c, speed, vehicle = (
            jnp.concatenate([inbox[s, 3 * p + low], inbox[s, 3 * p + high]], axis=0) for p in range(3)
        )
        used = c < EMPTY
        if h:
            used = used & (subs() < 4)
        made.append((jnp.where(used, SIGN | (c.astype(jnp.int32) << 16), 0), key_of(speed, vehicle)))
    return made


def spread_lists(inbox, s):
    x = []
    mask = SIGN | np.int32(3 << 27)
    for t in (s, s + 1):
        pair = short_list(inbox, t)
        for high in range(4):
            mine = SIGN | np.int32(high << 27)
            some = [(jnp.where((w & mask) == mine, w, 0), k) for w, k in pair]
            move_v(some, [(10, 0)])
            x += some
    move_s(x, [(9, 2), (8, 1), (7, 0)])
    x = turned(x)
    move_s(x, [(6, 2), (5, 1), (4, 0)])
    move_v(x, [(3, 3), (2, 2), (1, 1), (0, 0)])
    return [jnp.where(w < 0, k, -1) for w, k in x]


def joined(tables):
    best = tables[0]
    for t in tables[1:]:
        best = [jnp.maximum(a, b) for a, b in zip(best, t)]
    t = jnp.concatenate(best, axis=0).T
    return [jnp.maximum(t[8 * z : 8 * z + 8], t[64 + 8 * z : 72 + 8 * z]) for z in range(8)]


def exchange_kernel(cell, vehicle, speed, both, flags, A, B, out1, in1, out2, in2, out3, in3, mark, marks1, mark2,
                    marks2, send, recv):
    gx, gy = lax.axis_index("gx"), lax.axis_index("gy")
    y, z = gy // 8, gy % 8

    def peer(phase, j):
        if phase == 0:
            return (gx ^ j, gy)
        if phase == 1:
            return (gx, (y ^ j) * 8 + z)
        return (gx, y * 8 + (z ^ j))

    barrier = pltpu.get_barrier_semaphore()
    for phase in range(3):
        for j in range(1, 8):
            pl.semaphore_signal(barrier, inc=1, device_id=peer(phase, j), device_id_type=MESH)

    def copies(row, phase, source, target):
        return [
            pltpu.make_async_remote_copy(
                src_ref=source(j),
                dst_ref=target.at[j],
                send_sem=send.at[row, j],
                recv_sem=recv.at[row, j],
                device_id=peer(phase, j),
                device_id_type=MESH,
            )
            for j in range(1, 8)
        ]

    sort_events(cell, vehicle, speed, A, B)
    x, flag = compact_events(A, B)
    pack_messages(expand_lists(x), out1)
    pl.semaphore_wait(barrier, 21)
    first = copies(0, 0, lambda j: out1.at[gx ^ j], in1)
    for c in first:
        c.start()
    in1[0] = out1[gx]
    for c in first:
        c.wait_recv()

    x, more = regroup(merge_lists(in1))
    mark[...] = (flag | more).astype(jnp.float32)
    pack_short(x, out2)
    second = copies(1, 1, lambda j: out2.at[y ^ j], in2)
    for c in second:
        c.start()
    flags1 = copies(2, 0, lambda j: mark, marks1)
    for c in flags1:
        c.start()
    in2[0] = out2[y]
    for c in flags1:
        c.wait_recv()
    seen = mark[...]
    for j in range(1, 8):
        seen = jnp.maximum(seen, marks1[j])
    mark2[...] = seen
    flags2 = copies(3, 1, lambda j: mark2, marks2)
    for c in flags2:
        c.start()
    tables = []
    for s in range(0, 8, 2):
        for j in (s, s + 1):
            if j:
                second[j - 1].wait_recv()
        tables.append(spread_lists(in2, s))
    table = joined(tables)
    for c in flags2:
        c.wait_recv()
    for j in range(1, 8):
        seen = jnp.maximum(seen, marks2[j])
    for v, k in enumerate(table):
        there = k >= 0
        out3[v, 0] = jnp.where(there, (k >> 10).astype(jnp.float32) * (1.0 / 1024.0), -1.0)
        out3[v, 1] = jnp.where(there, (1023 - (k & 1023)).astype(jnp.float32), 1024.0) + seen * 4096.0
    third = copies(4, 2, lambda j: out3.at[z ^ j], in3)
    for c in third:
        c.start()
    in3[0] = out3[z]
    for c in third:
        c.wait_recv()
    k = key_of(in3[0, 0], in3[0, 1])
    most = in3[0, 1]
    for j in range(1, 8):
        k = jnp.maximum(k, key_of(in3[j, 0], in3[j, 1]))
        most = jnp.maximum(most, in3[j, 1])
    both[0] = jnp.where(k < 0, -1.0, (k >> 10).astype(jnp.float32) * (1.0 / 1024.0))
    both[1] = jnp.where(k < 0, -1, 1023 - (k & 1023)).astype(jnp.float32)
    flags[0, 0] = jnp.max(most).astype(jnp.int32)
    for group in (first, second, flags1, flags2, third):
        for c in group:
            c.wait_send()


def words(*shape):
    return pltpu.VMEM(shape + (8, 128), jnp.float32)


def sparse_path(cell, vehicle, speed):
    whole = pl.BlockSpec(memory_space=pltpu.VMEM)
    ints = lambda n: pltpu.VMEM((n, 8, 128), jnp.int32)
    return pl.pallas_call(
        exchange_kernel,
        out_shape=(
            jax.ShapeDtypeStruct((2, 8, 128), jnp.float32),
            jax.ShapeDtypeStruct((1, 1), jnp.int32),
        ),
        in_specs=[whole] * 3,
        out_specs=(whole, pl.BlockSpec(memory_space=pltpu.SMEM)),
        scratch_shapes=[
            ints(32), ints(32),
            words(8, 6), words(8, 6), pltpu.VMEM((8, 9, 4, 128), jnp.float32), pltpu.VMEM((8, 9, 4, 128), jnp.float32), words(8, 2), words(8, 2),
            words(), words(8), words(), words(8),
            pltpu.SemaphoreType.DMA((5, 8)),
            pltpu.SemaphoreType.DMA((5, 8)),
        ],
        compiler_params=pltpu.CompilerParams(collective_id=0, has_side_effects=True),
    )(cell, vehicle, speed)


def per_device(cell, vehicle, speed):
    shaped = [x.reshape(32, 8, 128) for x in (cell, vehicle, speed)]
    both, flags = sparse_path(*shaped)
    both = lax.cond(flags[0, 0] > 2048, lambda: dense_path(cell, vehicle, speed), lambda: both)
    return both[0].reshape(1024), both[1].astype(jnp.int32).reshape(1024)


def solution(mesh):
    placed = (P(("gx", "gy")), P(("gx", "gy")), P(("gx", "gy")))
    return jax.shard_map(
        per_device,
        mesh=mesh,
        in_specs=placed,
        out_specs=(P(("gx", "gy")), P(("gx", "gy"))),
        check_vma=False,
    )
```

```python
import jax
import jax.numpy as jnp
import numpy as np
from jax import lax
from jax.experimental import pallas as pl
from jax.experimental.pallas import tpu as pltpu
from jax.sharding import PartitionSpec as P

CELLS = 524288
VEHICLES = 1024
MESH = pl.DeviceIdType.MESH
FAR_FIRST = ((4, 5, 6, 7, 2, 3, 1), (4, 5, 3, 7, 6, 2, 1), (4, 5, 3, 7, 6, 2, 1))
SIGN = np.int32(-(2**31))
CAP = 2048
SHORT = 1536
EMPTY = 131072


def swapped(block, axis, apart):
    count = lax.axis_size(axis)
    route = []
    for low in range(count):
        high = low | 1 << apart
        if high != low and high < count:
            route += [(low, high), (high, low)]
    return lax.ppermute(block, axis, route)


def combine(first, second):
    speed_a = first[0]
    speed_b = second[0]
    best = jnp.maximum(speed_a, speed_b)
    ident = jnp.where(
        speed_a > speed_b,
        first[1],
        jnp.where(speed_b > speed_a, second[1], jnp.minimum(first[1], second[1])),
    )
    return jnp.stack([best, ident])


def dense_path(cell, vehicle, speed):
    local_best = jnp.full((CELLS,), -1.0, jnp.float32).at[cell].max(speed)
    chosen = jnp.where(speed == local_best[cell], vehicle, VEHICLES)
    local_ident = jnp.full((CELLS,), VEHICLES, jnp.int32).at[cell].min(chosen)
    paired = jnp.stack([local_best, local_ident.astype(jnp.float32)])
    outer = lax.axis_size("gx")
    inner = lax.axis_size("gy")
    nbits = (outer * inner).bit_length() - 1
    myself = lax.axis_index(("gx", "gy"))
    buffer = paired
    for level in reversed(range(nbits)):
        half = buffer.shape[1] // 2
        side = myself >> level & 1
        keep = lax.dynamic_slice_in_dim(buffer, side * half, half, 1)
        give = lax.dynamic_slice_in_dim(buffer, (1 - side) * half, half, 1)
        partner = swapped(give, ("gx", "gy"), level)
        buffer = combine(keep, partner)
    best = buffer[0]
    lowest = buffer[1].astype(jnp.int32)
    top_vehicle = jnp.where(lowest < VEHICLES, lowest, -1)
    return jnp.stack([best, top_vehicle.astype(jnp.float32)]).reshape(2, 8, 128)


def lanes():
    return lax.broadcasted_iota(jnp.int32, (8, 128), 1)


def subs():
    return lax.broadcasted_iota(jnp.int32, (8, 128), 0)


def lane_pick(x, index):
    return jnp.take_along_axis(x, index, axis=1)


def sub_pick(x, index):
    return jnp.take_along_axis(x, index, axis=0)


def sub_bit(i):
    return ((subs() >> i) & 1) == 1


def lane_bit(i):
    return ((lanes() >> i) & 1) == 1


def total_of(counts, matrix):
    return jnp.dot(counts, matrix, preferred_element_type=jnp.float32)


def above(x, y):
    tie = x[0] == y[0]
    return jnp.where(tie, x[1], x[0]) > jnp.where(tie, y[1], y[0])


def over(x, y):
    return x[0] > y[0]


def order_pair(a, b, down, more=above):
    swap = more(a, b)
    if down is True:
        a, b = b, a
    elif down is not False:
        swap = swap ^ down
    low = tuple(jnp.where(swap, y, x) for x, y in zip(a, b))
    high = tuple(jnp.where(swap, x, y) for x, y in zip(a, b))
    return low, high


def order_v(x, bits, down, more=above):
    for b in bits:
        for m in range(len(x)):
            if not m >> b & 1:
                x[m], x[m | 1 << b] = order_pair(x[m], x[m | 1 << b], down(m), more)


def order_cross(x, pick, index, bit, down, more):
    other = ~bit
    for m in range(len(x)):
        d = down(m)
        wants = bit if d is False else other if d is True else bit ^ d
        c, k = x[m]
        pc, pk = pick(c, index), pick(k, index)
        if more is above:
            swap = above((c, k), (pc, pk)) ^ wants
        else:
            turn = jnp.where(wants, -1, 0)
            swap = (c ^ turn) > (pc ^ turn)
        x[m] = jnp.where(swap, pc, c), jnp.where(swap, pk, k)


def order_s(x, bits, down, more=above):
    for i in bits:
        order_cross(x, sub_pick, subs() ^ (1 << i), sub_bit(i), down, more)


def order_l(x, bits, down, more=above):
    for i in bits:
        order_cross(x, lane_pick, lanes() ^ (1 << i), lane_bit(i), down, more)


def move_pair(a, b, bit):
    mask = SIGN | np.int32(1 << bit)
    ma, mb = a[0] & mask, b[0] & mask
    a0, b0 = ma == SIGN, mb == SIGN
    a1, b1 = ma == mask, mb == mask
    low = (jnp.where(b0, b[0], jnp.where(a0, a[0], 0)), jnp.where(b0, b[1], a[1]))
    high = (jnp.where(a1, a[0], jnp.where(b1, b[0], 0)), jnp.where(a1, a[1], b[1]))
    return low, high


def move_v(x, steps):
    for bit, i in steps:
        for m in range(len(x)):
            if not m >> i & 1:
                x[m], x[m | 1 << i] = move_pair(x[m], x[m | 1 << i], 16 + bit)


def move_s(x, steps):
    for bit, i in steps:
        b = 16 + bit
        mask = SIGN | np.int32(1 << b)
        here = SIGN | (((subs() >> i) & 1) << b)
        index = subs() ^ (1 << i)
        for m in range(len(x)):
            w, k = x[m]
            pw, pk = sub_pick(w, index), sub_pick(k, index)
            stay, come = (w & mask) == here, (pw & mask) == here
            x[m] = jnp.where(come, pw, jnp.where(stay, w, 0)), jnp.where(come, pk, k)


def turned(x):
    both = []
    for w in range(2):
        t = jnp.concatenate([p[w] for p in x], axis=0).T
        both.append([t[8 * m : 8 * m + 8] for m in range(16)])
    return list(zip(*both))


def batcher(n):
    pairs = []

    def merge(lo, n, r):
        m = r * 2
        if m < n:
            merge(lo, n, m)
            merge(lo + r, n, m)
            for i in range(lo + r, lo + n - r, m):
                pairs.append((i, i + r))
        else:
            pairs.append((lo, lo + r))

    def sort(lo, n):
        if n > 1:
            m = n // 2
            sort(lo, m)
            sort(lo + m, m)
            merge(lo, n, 1)

    sort(0, n)
    return pairs


def total(x):
    s = jnp.sum(x.astype(jnp.float32), axis=0, keepdims=True)
    s = jnp.sum(s, axis=1, keepdims=True)
    return jnp.broadcast_to(s, (8, 128)).astype(jnp.int32)


def sub_prefix(x):
    before, block = jnp.zeros_like(x), x
    for i in range(3):
        other = sub_pick(block, subs() ^ (1 << i))
        before = before + jnp.where(sub_bit(i), other, 0)
        block = block + other
    return before, block


def lane_prefix(x, order, places):
    row = lax.broadcasted_iota(jnp.int32, (128, 128), 0)
    column = lax.broadcasted_iota(jnp.int32, (128, 128), 1)
    x = x.astype(jnp.float32)
    before = [jnp.where(order(row) < place(column), 1.0, 0.0).astype(jnp.float32) for place in places]
    return [total_of(x, m).astype(jnp.int32) for m in before + [jnp.ones((128, 128), jnp.float32)]]


def load(A, B, at):
    return [(A[at + m], B[at + m]) for m in range(16)]


def save(A, B, at, x):
    for m in range(16):
        A[at + m] = x[m][0]
        B[at + m] = x[m][1]


def sort_events(cell, vehicle, speed, A, B):
    flip = -(subs() & 1)
    for block in (0, 16):
        x = []
        for m in range(16):
            c = cell[block + m]
            c = (c & 0x7FF80) | ((c & 7) << 4) | ((c >> 3) & 15)
            level = (speed[block + m] * 1024.0).astype(jnp.int32)
            w = ((c << 13) | (level >> 4)) ^ SIGN
            x.append((w ^ flip, ((level & 15) << 10) | (1023 - vehicle[block + m])))
        for i, j in batcher(16):
            x[i], x[j] = order_pair(x[i], x[j], False, over)
        x = [(w ^ flip, k) for w, k in x]
        for top in (1, 2, 3):
            way = sub_bit(top) if top < 3 else lane_bit(0)
            order_s(x, reversed(range(top)), lambda m: way, over)
            order_v(x, (3, 2, 1, 0), lambda m: way, over)
        save(A, B, block, x)
    for s in range(8, 16):
        if s > 10:
            for block in (0, 16):
                x = turned(load(A, B, block))
                order_v(x, reversed(range(s - 11)), lambda m: bool(m >> (s - 11) & 1), over)
                save(A, B, block, x)
            for m in range(16):
                pair = [(A[m], B[m]), (A[m + 16], B[m + 16])]
                order_v(pair, (0,), lambda _: bool(m >> (s - 11) & 1), over)
                for h in range(2):
                    A[m + 16 * h] = pair[h][0]
                    B[m + 16 * h] = pair[h][1]
        for block in (0, 16):
            x = load(A, B, block)
            way = lane_bit(s - 7) if s < 10 else block > 0 if s == 10 else lane_bit(s - 8) if s < 15 else False
            if s > 9:
                x = turned(x) if s == 10 else x
                order_s(x, (2, 1, 0), lambda m: way if s == 10 else bool(m >> (s - 11) & 1), over)
                x = turned(x)
            else:
                order_l(x, reversed(range(s - 7)), lambda m: way, over)
            order_s(x, (2, 1, 0), lambda m: way, over)
            order_v(x, (3, 2, 1, 0), lambda m: way, over)
            save(A, B, block, x)


def compact_events(A, B):
    lane, sub = lanes(), subs()
    first_edge = (lane & 7) == 0
    lows, ends, blocks = [], [], []
    for block in (0, 16):
        x = load(A, B, block)
        low = [x[0][1]]
        for m in range(1, 16):
            low.append(jnp.where(x[m][0] == x[m - 1][0], jnp.maximum(x[m][1], low[-1]), x[m][1]))
        blocks.append([w for w, _ in x])
        lows.append(low)
        ends.append((pltpu.roll(x[15][0], 1, 0), pltpu.roll(low[15], 1, 0)))
    beside = [tuple(pltpu.roll(t, 1, 1) for t in e) for e in ends]
    across = [beside[1], tuple(pltpu.roll(t, 121, 1) for t in ends[0])]
    flag = jnp.zeros((8, 128), jnp.int32)
    for h in range(2):
        w_before, k_before = (
            jnp.where(sub == 0, jnp.where(first_edge, far, near), own) for far, near, own in zip(across[h], beside[h], ends[h])
        )
        w = blocks[h]
        goes_on = w[0] == w_before
        flag = flag | (goes_on & (w[0] == w[15])).astype(jnp.int32)
        carry = jnp.where(goes_on, k_before, 0)
        lows[h] = [jnp.where(w[m] == w[0], jnp.maximum(lows[h][m], carry), lows[h][m]) for m in range(16)]
    cells = [[((w ^ SIGN) >> 13) & 0x7FFFF for w in blocks[h]] for h in range(2)]
    heads = [pltpu.roll(cells[h][0], 7, 0) for h in range(2)]
    nexts = [pltpu.roll(x, 127, 1) for x in heads]
    edge = (lane & 7) == 7
    follows = [
        jnp.where(sub == 7, jnp.where(edge, pltpu.roll(heads[1], 7, 1), nexts[0]), heads[0]),
        jnp.where(sub == 7, jnp.where(edge, nexts[0], nexts[1]), heads[1]),
    ]
    sums = []
    for h in range(2):
        run = jnp.zeros((8, 128), jnp.int32)
        x = []
        for m in range(16):
            c = cells[h][m]
            keep = c != (cells[h][m + 1] if m < 15 else follows[h])
            if h * 16 + m == 31:
                keep = keep | ((sub == 7) & (lane == 127))
            key = ((blocks[h][m] & 0x1FFF) << 14) | lows[h][m] | ((c >> 16) << 27)
            x.append((jnp.where(keep, SIGN | (run << 16) | (c & 0xFFFF), 0), key))
            run = run + keep.astype(jnp.int32)
        save(A, B, 16 * h, x)
        sums.append(sub_prefix(run))
    orders = [lambda l: ((l >> 3) << 4) + (l & 7), lambda l: ((l >> 3) << 4) + (l & 7) + 8]
    parts = [lane_prefix(sums[h][1], orders[h], orders) for h in range(2)]
    every = parts[0][2] + parts[1][2]
    for h in range(2):
        start = (parts[0][h] + parts[1][h] + sums[h][0]) << 16
        x = [(jnp.where(w < 0, w + start, 0), k) for w, k in load(A, B, 16 * h)]
        move_v(x, [(i, i) for i in range(4)])
        move_s(x, [(4 + i, i) for i in range(3)])
        x = turned(x)
        move_s(x, [(7 + i, i) for i in range(3)])
        save(A, B, 16 * h, x)
    for m in range(16):
        pair = move_pair((A[m], B[m]), (A[m + 16], B[m + 16]), 16 + 10)
        for h in range(2):
            A[m + 16 * h] = pair[h][0]
            B[m + 16 * h] = pair[h][1]
    y = []
    for h in range(2):
        x = load(A, B, 16 * h)
        move_v(x, [(11 + i, i) for i in range(4)])
        y += x[:8]
    starts = group_starts([k >> 27 for _, k in y], [w < 0 for w, _ in y])
    flag = flag | crowded(starts, CAP) | (every > 8 * CAP).astype(jnp.int32)
    y = aimed([(w, k & 0x7FFFFFF) for w, k in y], [k >> 27 for _, k in y], [w < 0 for w, _ in y], starts, 0xFFFF)
    return y, flag


def list_rank(v):
    lane = lanes()
    return (v & 7) * CAP + ((v >> 3) << 10) + (subs() << 7) + ((lane & 7) << 4) + (lane >> 3)


def group_starts(groups, valid):
    groups = [jnp.where(u, g, 8) for g, u in zip(groups, valid)]
    starts = [jnp.zeros((8, 128), jnp.int32)]
    for j in range(1, 9):
        t = jnp.zeros((8, 128), jnp.int32)
        for g in groups:
            t = t + jnp.where(g < j, 1, 0)
        starts.append(total(t))
    return starts


def crowded(starts, room):
    most = jnp.zeros((8, 128), jnp.int32)
    for j in range(8):
        most = jnp.maximum(most, starts[j + 1] - starts[j])
    return (most > room).astype(jnp.int32)


def aimed(x, groups, valid, starts, mask):
    made = []
    for v, (w, k) in enumerate(x):
        target = list_rank(v)
        moved = jnp.zeros((8, 128), jnp.int32)
        for j in range(1, 8):
            moved = jnp.where(groups[v] == j, j * CAP - starts[j], moved)
        made.append((jnp.where(valid[v], SIGN | ((target + moved) << 16) | (w & mask), 0), k))
    return made


def expand_lists(x):
    move_v(x, [(13, 2), (12, 1), (11, 0), (10, 3)])
    move_s(x, [(9, 2), (8, 1), (7, 0)])
    x = turned(x)
    move_s(x, [(6, 2), (5, 1), (4, 0)])
    move_v(x, [(3, 3), (2, 2), (1, 1), (0, 0)])
    return turned(x)


def planes(w, k):
    return (
        jnp.where(w < 0, w & 0xFFFF, EMPTY).astype(jnp.float32),
        (k >> 10).astype(jnp.float32) * (1.0 / 1024.0),
        (1023 - (k & 1023)).astype(jnp.float32),
    )


def pack_messages(x, out):
    for v, pair in enumerate(x):
        for p, plane in enumerate(planes(*pair)):
            out[v & 7, 2 * p + (v >> 3)] = plane


def pack_short(x, out):
    for v, pair in enumerate(x):
        for p, plane in enumerate(planes(*pair)):
            if v < 8:
                out[v, 3 * p] = plane[:4]
                out[v, 3 * p + 1] = plane[4:]
            else:
                out[v - 8, 3 * p + 2] = plane[:4]


def key_of(speed, vehicle):
    return (speed * 1024.0).astype(jnp.int32) * 1024 + (1023 - vehicle.astype(jnp.int32))


def merge_lists(inbox):
    around, back = 7 - subs(), 127 - lanes()
    x = [None] * 16
    for s in range(8):
        for h in range(2):
            pair = (inbox[s, h].astype(jnp.int32), key_of(inbox[s, 2 + h], inbox[s, 4 + h]))
            if s & 1:
                x[8 * (1 - h) + s] = tuple(lane_pick(sub_pick(w, around), back) for w in pair)
            else:
                x[8 * h + s] = pair
    for level in (1, 2, 3):
        down = (lambda m: bool(m >> level & 1)) if level < 3 else (lambda m: False)
        way = lane_bit(3 + level) if level < 3 else False
        order_v(x, (*reversed(range(level)), 3), down)
        order_s(x, (2, 1, 0), down)
        x = turned(x)
        order_s(x, (2, 1, 0), lambda m: way)
        order_v(x, (3, 2, 1, 0), lambda m: way)
        if level < 3:
            x = turned(x)
    return x


def best_of_cells(x):
    lane, sub = lanes(), subs()
    head = pltpu.roll(x[0][0], 7, 0)
    beyond = jnp.where(lane < 64, pltpu.roll(head, 71, 1), pltpu.roll(head, 63, 1))
    carried = jnp.where((lane & 7) == 7, beyond, pltpu.roll(head, 127, 1))
    follow = jnp.where(sub == 7, carried, head)
    run = jnp.zeros((8, 128), jnp.int32)
    y = []
    for m in range(16):
        c, k = x[m]
        keep = c != (x[m + 1][0] if m < 15 else follow)
        if m == 15:
            keep = keep | ((sub == 7) & (lane == 127))
        keep = keep & (c < EMPTY)
        y.append((jnp.where(keep, SIGN | (run << 16) | c, 0), k))
        run = run + keep.astype(jnp.int32)
    within, block = sub_prefix(run)
    order = lambda l: (((l >> 3) & 7) << 4) + ((l >> 6) << 3) + (l & 7)
    ahead = lane_prefix(block, order, [order])[0]
    start = (within + ahead) << 16
    y = [(jnp.where(w < 0, w + start, 0), k) for w, k in y]
    move_v(y, [(i, i) for i in range(4)])
    move_s(y, [(4 + i, i) for i in range(3)])
    y = turned(y)
    move_s(y, [(7 + i, i) for i in range(3)])
    move_v(y, [(10, 3), (11, 0), (12, 1), (13, 2)])
    return y


def regroup(x):
    y = best_of_cells(x)
    groups = [(w >> 13) & 7 for w, _ in y]
    valid = [w < 0 for w, _ in y]
    starts = group_starts(groups, valid)
    return expand_lists(aimed(y, groups, valid, starts, 0x1FFF)), crowded(starts, SHORT)


def short_list(inbox, s):
    made = []
    for h in range(2):
        low, high = (3 * h, 1) if h == 0 else (2, 2)
        c, speed, vehicle = (
            jnp.concatenate([inbox[s, 3 * p + low], inbox[s, 3 * p + high]], axis=0) for p in range(3)
        )
        used = c < EMPTY
        if h:
            used = used & (subs() < 4)
        made.append((jnp.where(used, SIGN | (c.astype(jnp.int32) << 16), 0), key_of(speed, vehicle)))
    return made


def spread_lists(inbox, pair):
    x = []
    mask = SIGN | np.int32(3 << 27)
    for s in pair:
        words = short_list(inbox, s)
        for high in range(4):
            mine = SIGN | np.int32(high << 27)
            some = [(jnp.where((w & mask) == mine, w, 0), k) for w, k in words]
            move_v(some, [(10, 0)])
            x += some
    move_s(x, [(9, 2), (8, 1), (7, 0)])
    x = turned(x)
    move_s(x, [(6, 2), (5, 1), (4, 0)])
    move_v(x, [(3, 3), (2, 2), (1, 1), (0, 0)])
    return [jnp.where(w < 0, k, -1) for w, k in x]


def joined(tables):
    best = tables[0]
    for t in tables[1:]:
        best = [jnp.maximum(a, b) for a, b in zip(best, t)]
    t = jnp.concatenate(best, axis=0).T
    return [jnp.maximum(t[8 * z : 8 * z + 8], t[64 + 8 * z : 72 + 8 * z]) for z in range(8)]


def exchange_kernel(cell, vehicle, speed, both, flags, A, B, out1, in1, out2, in2, out3, in3, mark, marks1, mark2,
                    marks2, send, recv):
    gx, gy = lax.axis_index("gx"), lax.axis_index("gy")
    y, z = gy // 8, gy % 8

    def peer(phase, j):
        if phase == 0:
            return (gx ^ j, gy)
        if phase == 1:
            return (gx, (y ^ j) * 8 + z)
        return (gx, y * 8 + (z ^ j))

    barrier = pltpu.get_barrier_semaphore()
    for phase in range(3):
        for j in range(1, 8):
            pl.semaphore_signal(barrier, inc=1, device_id=peer(phase, j), device_id_type=MESH)

    def copies(row, phase, source, target):
        return [
            pltpu.make_async_remote_copy(
                src_ref=source(j),
                dst_ref=target.at[j],
                send_sem=send.at[row, j],
                recv_sem=recv.at[row, j],
                device_id=peer(phase, j),
                device_id_type=MESH,
            )
            for j in FAR_FIRST[phase]
        ]

    sort_events(cell, vehicle, speed, A, B)
    x, flag = compact_events(A, B)
    pack_messages(expand_lists(x), out1)
    pl.semaphore_wait(barrier, 21)
    first = copies(0, 0, lambda j: out1.at[gx ^ j], in1)
    for c in first:
        c.start()
    in1[0] = out1[gx]
    for c in first:
        c.wait_recv()

    x, more = regroup(merge_lists(in1))
    mark[...] = (flag | more).astype(jnp.float32)
    pack_short(x, out2)
    second = copies(1, 1, lambda j: out2.at[y ^ j], in2)
    for c in second:
        c.start()
    flags1 = copies(2, 0, lambda j: mark, marks1)
    for c in flags1:
        c.start()
    in2[0] = out2[y]
    for c in flags1:
        c.wait_recv()
    seen = mark[...]
    for j in range(1, 8):
        seen = jnp.maximum(seen, marks1[j])
    mark2[...] = seen
    flags2 = copies(3, 1, lambda j: mark2, marks2)
    for c in flags2:
        c.start()
    tables = []
    for pair in ((0, 1), (2, 6), (3, 7), (4, 5)):
        for j in pair:
            if j:
                second[FAR_FIRST[1].index(j)].wait_recv()
        tables.append(spread_lists(in2, pair))
    table = joined(tables)
    for c in flags2:
        c.wait_recv()
    for j in range(1, 8):
        seen = jnp.maximum(seen, marks2[j])
    for v, k in enumerate(table):
        there = k >= 0
        out3[v, 0] = jnp.where(there, (k >> 10).astype(jnp.float32) * (1.0 / 1024.0), -1.0)
        out3[v, 1] = jnp.where(there, (1023 - (k & 1023)).astype(jnp.float32), 1024.0) + seen * 4096.0
    third = copies(4, 2, lambda j: out3.at[z ^ j], in3)
    for c in third:
        c.start()
    in3[0] = out3[z]
    for c in third:
        c.wait_recv()
    k = key_of(in3[0, 0], in3[0, 1])
    most = in3[0, 1]
    for j in range(1, 8):
        k = jnp.maximum(k, key_of(in3[j, 0], in3[j, 1]))
        most = jnp.maximum(most, in3[j, 1])
    both[0] = jnp.where(k < 0, -1.0, (k >> 10).astype(jnp.float32) * (1.0 / 1024.0))
    both[1] = jnp.where(k < 0, -1, 1023 - (k & 1023)).astype(jnp.float32)
    flags[0, 0] = jnp.max(most).astype(jnp.int32)
    for group in (first, second, flags1, flags2, third):
        for c in group:
            c.wait_send()


def words(*shape):
    return pltpu.VMEM(shape + (8, 128), jnp.float32)


def sparse_path(cell, vehicle, speed):
    whole = pl.BlockSpec(memory_space=pltpu.VMEM)
    ints = lambda n: pltpu.VMEM((n, 8, 128), jnp.int32)
    return pl.pallas_call(
        exchange_kernel,
        out_shape=(
            jax.ShapeDtypeStruct((2, 8, 128), jnp.float32),
            jax.ShapeDtypeStruct((1, 1), jnp.int32),
        ),
        in_specs=[whole] * 3,
        out_specs=(whole, pl.BlockSpec(memory_space=pltpu.SMEM)),
        scratch_shapes=[
            ints(32), ints(32),
            words(8, 6), words(8, 6), pltpu.VMEM((8, 9, 4, 128), jnp.float32), pltpu.VMEM((8, 9, 4, 128), jnp.float32), words(8, 2), words(8, 2),
            words(), words(8), words(), words(8),
            pltpu.SemaphoreType.DMA((5, 8)),
            pltpu.SemaphoreType.DMA((5, 8)),
        ],
        compiler_params=pltpu.CompilerParams(collective_id=0, has_side_effects=True),
    )(cell, vehicle, speed)


def per_device(cell, vehicle, speed):
    shaped = [x.reshape(32, 8, 128) for x in (cell, vehicle, speed)]
    both, flags = sparse_path(*shaped)
    both = lax.cond(flags[0, 0] > 2048, lambda: dense_path(cell, vehicle, speed), lambda: both)
    return both[0].reshape(1024), both[1].astype(jnp.int32).reshape(1024)


def solution(mesh):
    placed = (P(("gx", "gy")), P(("gx", "gy")), P(("gx", "gy")))
    return jax.shard_map(
        per_device,
        mesh=mesh,
        in_specs=placed,
        out_specs=(P(("gx", "gy")), P(("gx", "gy"))),
        check_vma=False,
    )
```

```python
import jax
import jax.numpy as jnp
import numpy as np
from jax import lax
from jax.experimental import pallas as pl
from jax.experimental.pallas import tpu as pltpu
from jax.sharding import PartitionSpec as P

CELLS = 524288
VEHICLES = 1024
MESH = pl.DeviceIdType.MESH
FAR_FIRST = ((4, 5, 6, 7, 2, 3, 1), (4, 5, 3, 7, 6, 2, 1), (4, 5, 3, 7, 6, 2, 1))
SIGN = np.int32(-(2**31))
CAP = 2048
SHORT = 1536
EMPTY = 131072


def swapped(block, axis, apart):
    count = lax.axis_size(axis)
    route = []
    for low in range(count):
        high = low | 1 << apart
        if high != low and high < count:
            route += [(low, high), (high, low)]
    return lax.ppermute(block, axis, route)


def combine(first, second):
    speed_a = first[0]
    speed_b = second[0]
    best = jnp.maximum(speed_a, speed_b)
    ident = jnp.where(
        speed_a > speed_b,
        first[1],
        jnp.where(speed_b > speed_a, second[1], jnp.minimum(first[1], second[1])),
    )
    return jnp.stack([best, ident])


def dense_path(cell, vehicle, speed):
    local_best = jnp.full((CELLS,), -1.0, jnp.float32).at[cell].max(speed)
    chosen = jnp.where(speed == local_best[cell], vehicle, VEHICLES)
    local_ident = jnp.full((CELLS,), VEHICLES, jnp.int32).at[cell].min(chosen)
    paired = jnp.stack([local_best, local_ident.astype(jnp.float32)])
    outer = lax.axis_size("gx")
    inner = lax.axis_size("gy")
    nbits = (outer * inner).bit_length() - 1
    myself = lax.axis_index(("gx", "gy"))
    buffer = paired
    for level in reversed(range(nbits)):
        half = buffer.shape[1] // 2
        side = myself >> level & 1
        keep = lax.dynamic_slice_in_dim(buffer, side * half, half, 1)
        give = lax.dynamic_slice_in_dim(buffer, (1 - side) * half, half, 1)
        partner = swapped(give, ("gx", "gy"), level)
        buffer = combine(keep, partner)
    best = buffer[0]
    lowest = buffer[1].astype(jnp.int32)
    top_vehicle = jnp.where(lowest < VEHICLES, lowest, -1)
    return jnp.stack([best, top_vehicle.astype(jnp.float32)]).reshape(2, 8, 128)


def lanes():
    return lax.broadcasted_iota(jnp.int32, (8, 128), 1)


def subs():
    return lax.broadcasted_iota(jnp.int32, (8, 128), 0)


def lane_pick(x, index):
    return jnp.take_along_axis(x, index, axis=1)


def sub_pick(x, index):
    return jnp.take_along_axis(x, index, axis=0)


def sub_bit(i):
    return ((subs() >> i) & 1) == 1


def lane_bit(i):
    return ((lanes() >> i) & 1) == 1


def total_of(counts, matrix):
    return jnp.dot(counts, matrix, preferred_element_type=jnp.float32)


def above(x, y):
    tie = x[0] == y[0]
    return jnp.where(tie, x[1], x[0]) > jnp.where(tie, y[1], y[0])


def over(x, y):
    return x[0] > y[0]


def order_pair(a, b, down, more=above):
    swap = more(a, b)
    if down is True:
        a, b = b, a
    elif down is not False:
        swap = swap ^ down
    low = tuple(jnp.where(swap, y, x) for x, y in zip(a, b))
    high = tuple(jnp.where(swap, x, y) for x, y in zip(a, b))
    return low, high


def order_v(x, bits, down, more=above):
    for b in bits:
        for m in range(len(x)):
            if not m >> b & 1:
                x[m], x[m | 1 << b] = order_pair(x[m], x[m | 1 << b], down(m), more)


def order_cross(x, pick, index, bit, down, more):
    other = ~bit
    for m in range(len(x)):
        d = down(m)
        wants = bit if d is False else other if d is True else bit ^ d
        c, k = x[m]
        pc, pk = pick(c, index), pick(k, index)
        if more is above:
            swap = above((c, k), (pc, pk)) ^ wants
        else:
            turn = jnp.where(wants, -1, 0)
            swap = (c ^ turn) > (pc ^ turn)
        x[m] = jnp.where(swap, pc, c), jnp.where(swap, pk, k)


def order_s(x, bits, down, more=above):
    for i in bits:
        order_cross(x, sub_pick, subs() ^ (1 << i), sub_bit(i), down, more)


def order_l(x, bits, down, more=above):
    for i in bits:
        order_cross(x, lane_pick, lanes() ^ (1 << i), lane_bit(i), down, more)


def move_pair(a, b, bit):
    mask = SIGN | np.int32(1 << bit)
    ma, mb = a[0] & mask, b[0] & mask
    a0, b0 = ma == SIGN, mb == SIGN
    a1, b1 = ma == mask, mb == mask
    low = (jnp.where(b0, b[0], jnp.where(a0, a[0], 0)), jnp.where(b0, b[1], a[1]))
    high = (jnp.where(a1, a[0], jnp.where(b1, b[0], 0)), jnp.where(a1, a[1], b[1]))
    return low, high


def move_v(x, steps):
    for bit, i in steps:
        for m in range(len(x)):
            if not m >> i & 1:
                x[m], x[m | 1 << i] = move_pair(x[m], x[m | 1 << i], 16 + bit)


def move_s(x, steps):
    for bit, i in steps:
        b = 16 + bit
        mask = SIGN | np.int32(1 << b)
        here = SIGN | (((subs() >> i) & 1) << b)
        index = subs() ^ (1 << i)
        for m in range(len(x)):
            w, k = x[m]
            pw, pk = sub_pick(w, index), sub_pick(k, index)
            stay, come = (w & mask) == here, (pw & mask) == here
            x[m] = jnp.where(come, pw, jnp.where(stay, w, 0)), jnp.where(come, pk, k)


def turned(x):
    both = []
    for w in range(2):
        t = jnp.concatenate([p[w] for p in x], axis=0).T
        both.append([t[8 * m : 8 * m + 8] for m in range(16)])
    return list(zip(*both))


def batcher(n):
    pairs = []

    def merge(lo, n, r):
        m = r * 2
        if m < n:
            merge(lo, n, m)
            merge(lo + r, n, m)
            for i in range(lo + r, lo + n - r, m):
                pairs.append((i, i + r))
        else:
            pairs.append((lo, lo + r))

    def sort(lo, n):
        if n > 1:
            m = n // 2
            sort(lo, m)
            sort(lo + m, m)
            merge(lo, n, 1)

    sort(0, n)
    return pairs


def total(x):
    s = jnp.sum(x.astype(jnp.float32), axis=0, keepdims=True)
    s = jnp.sum(s, axis=1, keepdims=True)
    return jnp.broadcast_to(s, (8, 128)).astype(jnp.int32)


def sub_prefix(x):
    before, block = jnp.zeros_like(x), x
    for i in range(3):
        other = sub_pick(block, subs() ^ (1 << i))
        before = before + jnp.where(sub_bit(i), other, 0)
        block = block + other
    return before, block


def lane_prefix(x, order, places):
    row = lax.broadcasted_iota(jnp.int32, (128, 128), 0)
    column = lax.broadcasted_iota(jnp.int32, (128, 128), 1)
    x = x.astype(jnp.float32)
    before = [jnp.where(order(row) < place(column), 1.0, 0.0).astype(jnp.float32) for place in places]
    return [total_of(x, m).astype(jnp.int32) for m in before + [jnp.ones((128, 128), jnp.float32)]]


def load(A, B, at):
    return [(A[at + m], B[at + m]) for m in range(16)]


def save(A, B, at, x):
    for m in range(16):
        A[at + m] = x[m][0]
        B[at + m] = x[m][1]


def sort_events(cell, vehicle, speed, A, B):
    flip = -(subs() & 1)
    for block in (0, 16):
        x = []
        for m in range(16):
            c = cell[block + m]
            c = (c & 0x7FF80) | ((c & 7) << 4) | ((c >> 3) & 15)
            level = (speed[block + m] * 1024.0).astype(jnp.int32)
            w = ((c << 13) | (level >> 4)) ^ SIGN
            x.append((w ^ flip, ((level & 15) << 10) | (1023 - vehicle[block + m])))
        for i, j in batcher(16):
            x[i], x[j] = order_pair(x[i], x[j], False, over)
        x = [(w ^ flip, k) for w, k in x]
        for top in (1, 2, 3):
            way = sub_bit(top) if top < 3 else lane_bit(0)
            order_s(x, reversed(range(top)), lambda m: way, over)
            order_v(x, (3, 2, 1, 0), lambda m: way, over)
        save(A, B, block, x)
    for s in range(8, 16):
        if s > 10:
            for block in (0, 16):
                x = turned(load(A, B, block))
                order_v(x, reversed(range(s - 11)), lambda m: bool(m >> (s - 11) & 1), over)
                save(A, B, block, x)
            for m in range(16):
                pair = [(A[m], B[m]), (A[m + 16], B[m + 16])]
                order_v(pair, (0,), lambda _: bool(m >> (s - 11) & 1), over)
                for h in range(2):
                    A[m + 16 * h] = pair[h][0]
                    B[m + 16 * h] = pair[h][1]
        for block in (0, 16):
            x = load(A, B, block)
            way = lane_bit(s - 7) if s < 10 else block > 0 if s == 10 else lane_bit(s - 8) if s < 15 else False
            if s > 9:
                x = turned(x) if s == 10 else x
                order_s(x, (2, 1, 0), lambda m: way if s == 10 else bool(m >> (s - 11) & 1), over)
                x = turned(x)
            else:
                order_l(x, reversed(range(s - 7)), lambda m: way, over)
            order_s(x, (2, 1, 0), lambda m: way, over)
            order_v(x, (3, 2, 1, 0), lambda m: way, over)
            save(A, B, block, x)


def compact_events(A, B):
    lane, sub = lanes(), subs()
    first_edge = (lane & 7) == 0
    lows, ends, blocks = [], [], []
    for block in (0, 16):
        x = load(A, B, block)
        low = [x[0][1]]
        for m in range(1, 16):
            low.append(jnp.where(x[m][0] == x[m - 1][0], jnp.maximum(x[m][1], low[-1]), x[m][1]))
        blocks.append([w for w, _ in x])
        lows.append(low)
        ends.append((pltpu.roll(x[15][0], 1, 0), pltpu.roll(low[15], 1, 0)))
    beside = [tuple(pltpu.roll(t, 1, 1) for t in e) for e in ends]
    across = [beside[1], tuple(pltpu.roll(t, 121, 1) for t in ends[0])]
    flag = jnp.zeros((8, 128), jnp.int32)
    for h in range(2):
        w_before, k_before = (
            jnp.where(sub == 0, jnp.where(first_edge, far, near), own) for far, near, own in zip(across[h], beside[h], ends[h])
        )
        w = blocks[h]
        goes_on = w[0] == w_before
        flag = flag | (goes_on & (w[0] == w[15])).astype(jnp.int32)
        carry = jnp.where(goes_on, k_before, 0)
        lows[h] = [jnp.where(w[m] == w[0], jnp.maximum(lows[h][m], carry), lows[h][m]) for m in range(16)]
    cells = [[((w ^ SIGN) >> 13) & 0x7FFFF for w in blocks[h]] for h in range(2)]
    heads = [pltpu.roll(cells[h][0], 7, 0) for h in range(2)]
    nexts = [pltpu.roll(x, 127, 1) for x in heads]
    edge = (lane & 7) == 7
    follows = [
        jnp.where(sub == 7, jnp.where(edge, pltpu.roll(heads[1], 7, 1), nexts[0]), heads[0]),
        jnp.where(sub == 7, jnp.where(edge, nexts[0], nexts[1]), heads[1]),
    ]
    sums, keeps = [], []
    for h in range(2):
        run = jnp.zeros((8, 128), jnp.int32)
        x = []
        for m in range(16):
            c = cells[h][m]
            keep = c != (cells[h][m + 1] if m < 15 else follows[h])
            if h * 16 + m == 31:
                keep = keep | ((sub == 7) & (lane == 127))
            keeps.append(keep)
            key = ((blocks[h][m] & 0x1FFF) << 14) | lows[h][m] | ((c >> 16) << 27)
            x.append((jnp.where(keep, SIGN | (run << 16) | (c & 0xFFFF), 0), key))
            run = run + keep.astype(jnp.int32)
        save(A, B, 16 * h, x)
        sums.append(sub_prefix(run))
    orders = [lambda l: ((l >> 3) << 4) + (l & 7), lambda l: ((l >> 3) << 4) + (l & 7) + 8]
    parts = [lane_prefix(sums[h][1], orders[h], orders) for h in range(2)]
    every = parts[0][2] + parts[1][2]
    starts = group_starts(cells[0] + cells[1], keeps, every, 16)
    for h in range(2):
        ahead = (parts[0][h] + parts[1][h] + sums[h][0]) << 16
        x = [(jnp.where(w < 0, w + ahead, 0), k) for w, k in load(A, B, 16 * h)]
        move_v(x, [(i, i) for i in range(4)])
        move_s(x, [(4 + i, i) for i in range(3)])
        x = turned(x)
        move_s(x, [(7 + i, i) for i in range(3)])
        save(A, B, 16 * h, x)
    for m in range(16):
        pair = move_pair((A[m], B[m]), (A[m + 16], B[m + 16]), 16 + 10)
        for h in range(2):
            A[m + 16 * h] = pair[h][0]
            B[m + 16 * h] = pair[h][1]
    y = []
    for h in range(2):
        x = load(A, B, 16 * h)
        move_v(x, [(11 + i, i) for i in range(4)])
        y += x[:8]
    flag = flag | crowded(starts, CAP) | (every > 8 * CAP).astype(jnp.int32)
    y = aimed([(w, k & 0x7FFFFFF) for w, k in y], [k >> 27 for _, k in y], [w < 0 for w, _ in y], starts, 0xFFFF)
    return y, flag


def list_rank(v):
    lane = lanes()
    return (v & 7) * CAP + ((v >> 3) << 10) + (subs() << 7) + ((lane & 7) << 4) + (lane >> 3)


def group_starts(cells, keeps, every, shift):
    cells = [jnp.where(u, c, CELLS) for c, u in zip(cells, keeps)]
    starts = [jnp.zeros((8, 128), jnp.int32)]
    for j in range(1, 8):
        t = jnp.zeros((8, 128), jnp.int32)
        for c in cells:
            t = t + jnp.where(c < j << shift, 1, 0)
        starts.append(total(t))
    return starts + [every]


def crowded(starts, room):
    most = jnp.zeros((8, 128), jnp.int32)
    for j in range(8):
        most = jnp.maximum(most, starts[j + 1] - starts[j])
    return (most > room).astype(jnp.int32)


def aimed(x, groups, valid, starts, mask):
    made = []
    for v, (w, k) in enumerate(x):
        target = list_rank(v)
        moved = jnp.zeros((8, 128), jnp.int32)
        for j in range(1, 8):
            moved = jnp.where(groups[v] == j, j * CAP - starts[j], moved)
        made.append((jnp.where(valid[v], SIGN | ((target + moved) << 16) | (w & mask), 0), k))
    return made


def expand_lists(x):
    move_v(x, [(13, 2), (12, 1), (11, 0), (10, 3)])
    move_s(x, [(9, 2), (8, 1), (7, 0)])
    x = turned(x)
    move_s(x, [(6, 2), (5, 1), (4, 0)])
    move_v(x, [(3, 3), (2, 2), (1, 1), (0, 0)])
    return turned(x)


def planes(w, k):
    return (
        jnp.where(w < 0, w & 0xFFFF, EMPTY).astype(jnp.float32),
        (k >> 10).astype(jnp.float32) * (1.0 / 1024.0),
        (1023 - (k & 1023)).astype(jnp.float32),
    )


def pack_messages(x, out):
    for v, pair in enumerate(x):
        for p, plane in enumerate(planes(*pair)):
            out[v & 7, 2 * p + (v >> 3)] = plane


def pack_short(x, out):
    for v, pair in enumerate(x):
        for p, plane in enumerate(planes(*pair)):
            if v < 8:
                out[v, 3 * p] = plane[:4]
                out[v, 3 * p + 1] = plane[4:]
            else:
                out[v - 8, 3 * p + 2] = plane[:4]


def key_of(speed, vehicle):
    return (speed * 1024.0).astype(jnp.int32) * 1024 + (1023 - vehicle.astype(jnp.int32))


def merge_lists(inbox):
    around, back = 7 - subs(), 127 - lanes()
    x = [None] * 16
    for s in range(8):
        for h in range(2):
            pair = (inbox[s, h].astype(jnp.int32), key_of(inbox[s, 2 + h], inbox[s, 4 + h]))
            if s & 1:
                x[8 * (1 - h) + s] = tuple(lane_pick(sub_pick(w, around), back) for w in pair)
            else:
                x[8 * h + s] = pair
    for level in (1, 2, 3):
        down = (lambda m: bool(m >> level & 1)) if level < 3 else (lambda m: False)
        way = lane_bit(3 + level) if level < 3 else False
        order_v(x, (*reversed(range(level)), 3), down)
        order_s(x, (2, 1, 0), down)
        x = turned(x)
        order_s(x, (2, 1, 0), lambda m: way)
        order_v(x, (3, 2, 1, 0), lambda m: way)
        if level < 3:
            x = turned(x)
    return x


def best_of_cells(x, tell):
    lane, sub = lanes(), subs()
    head = pltpu.roll(x[0][0], 7, 0)
    beyond = jnp.where(lane < 64, pltpu.roll(head, 71, 1), pltpu.roll(head, 63, 1))
    carried = jnp.where((lane & 7) == 7, beyond, pltpu.roll(head, 127, 1))
    follow = jnp.where(sub == 7, carried, head)
    run = jnp.zeros((8, 128), jnp.int32)
    y, keeps = [], []
    for m in range(16):
        c, k = x[m]
        keep = c != (x[m + 1][0] if m < 15 else follow)
        if m == 15:
            keep = keep | ((sub == 7) & (lane == 127))
        keep = keep & (c < EMPTY)
        keeps.append(keep)
        y.append((jnp.where(keep, SIGN | (run << 16) | c, 0), k))
        run = run + keep.astype(jnp.int32)
    within, block = sub_prefix(run)
    order = lambda l: (((l >> 3) & 7) << 4) + ((l >> 6) << 3) + (l & 7)
    ahead, every = lane_prefix(block, order, [order])
    starts = group_starts([c for c, _ in x], keeps, every, 13)
    tell(crowded(starts, SHORT))
    start = (within + ahead) << 16
    y = [(jnp.where(w < 0, w + start, 0), k) for w, k in y]
    move_v(y, [(i, i) for i in range(4)])
    move_s(y, [(4 + i, i) for i in range(3)])
    y = turned(y)
    move_s(y, [(7 + i, i) for i in range(3)])
    move_v(y, [(10, 3), (11, 0), (12, 1), (13, 2)])
    return y, starts


def regroup(x, tell):
    y, starts = best_of_cells(x, tell)
    groups = [(w >> 13) & 7 for w, _ in y]
    valid = [w < 0 for w, _ in y]
    return expand_lists(aimed(y, groups, valid, starts, 0x1FFF))


def short_list(inbox, s):
    made = []
    for h in range(2):
        low, high = (3 * h, 1) if h == 0 else (2, 2)
        c, speed, vehicle = (
            jnp.concatenate([inbox[s, 3 * p + low], inbox[s, 3 * p + high]], axis=0) for p in range(3)
        )
        used = c < EMPTY
        if h:
            used = used & (subs() < 4)
        made.append((jnp.where(used, SIGN | (c.astype(jnp.int32) << 16), 0), key_of(speed, vehicle)))
    return made


def spread_lists(inbox, pair):
    x = []
    mask = SIGN | np.int32(3 << 27)
    for s in pair:
        words = short_list(inbox, s)
        for high in range(4):
            mine = SIGN | np.int32(high << 27)
            some = [(jnp.where((w & mask) == mine, w, 0), k) for w, k in words]
            move_v(some, [(10, 0)])
            x += some
    move_s(x, [(9, 2), (8, 1), (7, 0)])
    x = turned(x)
    move_s(x, [(6, 2), (5, 1), (4, 0)])
    move_v(x, [(3, 3), (2, 2), (1, 1), (0, 0)])
    return [jnp.where(w < 0, k, -1) for w, k in x]


def joined(tables):
    best = tables[0]
    for t in tables[1:]:
        best = [jnp.maximum(a, b) for a, b in zip(best, t)]
    t = jnp.concatenate(best, axis=0).T
    return [jnp.maximum(t[8 * z : 8 * z + 8], t[64 + 8 * z : 72 + 8 * z]) for z in range(8)]


def exchange_kernel(cell, vehicle, speed, both, flags, events, reals, A, B, out1, in1, out2, in2, out3, in3, mark, marks,
                    arrive, send, recv):
    gx, gy = lax.axis_index("gx"), lax.axis_index("gy")
    y, z = gy // 8, gy % 8
    loads = [
        pltpu.make_async_copy(cell, events.at[0], arrive.at[0]),
        pltpu.make_async_copy(vehicle, events.at[1], arrive.at[1]),
        pltpu.make_async_copy(speed, reals, arrive.at[2]),
    ]
    for c in loads:
        c.start()

    def peer(phase, j):
        if phase == 0:
            return (gx ^ j, gy)
        if phase == 1:
            return (gx, (y ^ j) * 8 + z)
        return (gx, y * 8 + (z ^ j))

    barrier = pltpu.get_barrier_semaphore()
    for phase in range(3):
        for j in range(1, 8):
            pl.semaphore_signal(barrier, inc=1, device_id=peer(phase, j), device_id_type=MESH)

    def copies(row, phase, source, target):
        return [
            pltpu.make_async_remote_copy(
                src_ref=source(j),
                dst_ref=target(j),
                send_sem=send.at[row, j],
                recv_sem=recv.at[row, j],
                device_id=peer(phase, j),
                device_id_type=MESH,
            )
            for j in FAR_FIRST[phase]
        ]

    def share(phase, seen):
        mark[phase] = seen
        made = copies(3 + phase, phase, lambda j: mark.at[phase], lambda j: marks.at[phase, j])
        for c in made:
            c.start()
        return made

    def seen_by(phase, made, seen):
        for c in made:
            c.wait_recv()
        for j in range(1, 8):
            seen = jnp.maximum(seen, marks[phase, j])
        return seen

    for c in loads:
        c.wait()
    sort_events(events.at[0], events.at[1], reals, A, B)
    x, flag = compact_events(A, B)
    pack_messages(expand_lists(x), out1)
    pl.semaphore_wait(barrier, 21)
    first = copies(0, 0, lambda j: out1.at[gx ^ j], lambda j: in1.at[j])
    for c in first:
        c.start()
    in1[0] = out1[gx]
    for c in first:
        c.wait_recv()

    told = []

    def tell(more):
        seen = jnp.max((flag | more).astype(jnp.float32), axis=0, keepdims=True)
        told.append((share(0, seen), seen))

    x = regroup(merge_lists(in1), tell)
    pack_short(x, out2)
    second = copies(1, 1, lambda j: out2.at[y ^ j], lambda j: in2.at[j])
    for c in second:
        c.start()
    in2[0] = out2[y]
    seen = seen_by(0, *told[0])
    told.append((share(2, seen), seen))

    tables = []
    for pair in ((0, 1), (2, 6), (3, 7), (4, 5)):
        for j in pair:
            if j:
                second[FAR_FIRST[1].index(j)].wait_recv()
        tables.append(spread_lists(in2, pair))
    for v, k in enumerate(joined(tables)):
        there = k >= 0
        out3[v, 0] = jnp.where(there, (k >> 10).astype(jnp.float32) * (1.0 / 1024.0), -1.0)
        out3[v, 1] = jnp.where(there, (1023 - (k & 1023)).astype(jnp.float32), 1024.0)
    third = copies(2, 2, lambda j: out3.at[z ^ j], lambda j: in3.at[j])
    for c in third:
        c.start()
    seen = seen_by(2, *told[1])
    told.append((share(1, seen), seen))
    in3[0] = out3[z]
    k = key_of(in3[0, 0], in3[0, 1])
    for j in reversed(FAR_FIRST[2]):
        third[FAR_FIRST[2].index(j)].wait_recv()
        k = jnp.maximum(k, key_of(in3[j, 0], in3[j, 1]))
    both[0] = jnp.where(k < 0, -1.0, (k >> 10).astype(jnp.float32) * (1.0 / 1024.0))
    both[1] = jnp.where(k < 0, -1, 1023 - (k & 1023)).astype(jnp.float32)
    flags[0, 0] = jnp.max(seen_by(1, *told[2])).astype(jnp.int32)
    for group in (first, second, third, *(made for made, _ in told)):
        for c in group:
            c.wait_send()


def words(*shape):
    return pltpu.VMEM(shape + (8, 128), jnp.float32)


def sparse_path(cell, vehicle, speed):
    whole = pl.BlockSpec(memory_space=pltpu.VMEM)
    ints = lambda n: pltpu.VMEM((n, 8, 128), jnp.int32)
    return pl.pallas_call(
        exchange_kernel,
        out_shape=(
            jax.ShapeDtypeStruct((2, 8, 128), jnp.float32),
            jax.ShapeDtypeStruct((1, 1), jnp.int32),
        ),
        in_specs=[pl.BlockSpec(memory_space=pl.ANY)] * 3,
        out_specs=(whole, pl.BlockSpec(memory_space=pltpu.SMEM)),
        scratch_shapes=[
            pltpu.VMEM((2, 32, 8, 128), jnp.int32),
            words(32),
            ints(32),
            ints(32),
            words(8, 6),
            words(8, 6),
            pltpu.VMEM((8, 9, 4, 128), jnp.float32),
            pltpu.VMEM((8, 9, 4, 128), jnp.float32),
            words(8, 2),
            words(8, 2),
            pltpu.VMEM((3, 1, 128), jnp.float32),
            pltpu.VMEM((3, 8, 1, 128), jnp.float32),
            pltpu.SemaphoreType.DMA((3,)),
            pltpu.SemaphoreType.DMA((6, 8)),
            pltpu.SemaphoreType.DMA((6, 8)),
        ],
        compiler_params=pltpu.CompilerParams(collective_id=0, has_side_effects=True),
    )(cell, vehicle, speed)


def per_device(cell, vehicle, speed):
    shaped = [x.reshape(32, 8, 128) for x in (cell, vehicle, speed)]
    both, flags = sparse_path(*shaped)
    both = lax.cond(flags[0, 0] > 0, lambda: dense_path(cell, vehicle, speed), lambda: both)
    return both[0].reshape(1024), both[1].astype(jnp.int32).reshape(1024)


def solution(mesh):
    placed = (P(("gx", "gy")), P(("gx", "gy")), P(("gx", "gy")))
    return jax.shard_map(
        per_device,
        mesh=mesh,
        in_specs=placed,
        out_specs=(P(("gx", "gy")), P(("gx", "gy"))),
        check_vma=False,
    )
```

```python
import jax
import jax.numpy as jnp
import numpy as np
from jax import lax
from jax.experimental import pallas as pl
from jax.experimental.pallas import tpu as pltpu
from jax.sharding import PartitionSpec as P

CELLS = 524288
VEHICLES = 1024
MESH = pl.DeviceIdType.MESH
FAR_FIRST = ((4, 5, 6, 7, 2, 3, 1), (4, 5, 3, 7, 6, 2, 1), (4, 5, 3, 7, 6, 2, 1))
SIGN = np.int32(-(2**31))
CAP = 2048
SHORT = 1536
EMPTY = 131072


def swapped(block, axis, apart):
    count = lax.axis_size(axis)
    route = []
    for low in range(count):
        high = low | 1 << apart
        if high != low and high < count:
            route += [(low, high), (high, low)]
    return lax.ppermute(block, axis, route)


def combine(first, second):
    speed_a = first[0]
    speed_b = second[0]
    best = jnp.maximum(speed_a, speed_b)
    ident = jnp.where(
        speed_a > speed_b,
        first[1],
        jnp.where(speed_b > speed_a, second[1], jnp.minimum(first[1], second[1])),
    )
    return jnp.stack([best, ident])


def dense_path(cell, vehicle, speed):
    local_best = jnp.full((CELLS,), -1.0, jnp.float32).at[cell].max(speed)
    chosen = jnp.where(speed == local_best[cell], vehicle, VEHICLES)
    local_ident = jnp.full((CELLS,), VEHICLES, jnp.int32).at[cell].min(chosen)
    paired = jnp.stack([local_best, local_ident.astype(jnp.float32)])
    outer = lax.axis_size("gx")
    inner = lax.axis_size("gy")
    nbits = (outer * inner).bit_length() - 1
    myself = lax.axis_index(("gx", "gy"))
    buffer = paired
    for level in reversed(range(nbits)):
        half = buffer.shape[1] // 2
        side = myself >> level & 1
        keep = lax.dynamic_slice_in_dim(buffer, side * half, half, 1)
        give = lax.dynamic_slice_in_dim(buffer, (1 - side) * half, half, 1)
        partner = swapped(give, ("gx", "gy"), level)
        buffer = combine(keep, partner)
    best = buffer[0]
    lowest = buffer[1].astype(jnp.int32)
    top_vehicle = jnp.where(lowest < VEHICLES, lowest, -1)
    return jnp.stack([best, top_vehicle.astype(jnp.float32)]).reshape(2, 8, 128)


def lanes():
    return lax.broadcasted_iota(jnp.int32, (8, 128), 1)


def subs():
    return lax.broadcasted_iota(jnp.int32, (8, 128), 0)


def lane_pick(x, index):
    return jnp.take_along_axis(x, index, axis=1)


def sub_pick(x, index):
    return jnp.take_along_axis(x, index, axis=0)


def sub_bit(i):
    return ((subs() >> i) & 1) == 1


def lane_bit(i):
    return ((lanes() >> i) & 1) == 1


def total_of(counts, matrix):
    return jnp.dot(counts, matrix, preferred_element_type=jnp.float32)


def above(x, y):
    tie = x[0] == y[0]
    return jnp.where(tie, x[1], x[0]) > jnp.where(tie, y[1], y[0])


def over(x, y):
    return x[0] > y[0]


def order_pair(a, b, down, more=above):
    swap = more(a, b)
    if down is True:
        a, b = b, a
    elif down is not False:
        swap = swap ^ down
    low = tuple(jnp.where(swap, y, x) for x, y in zip(a, b))
    high = tuple(jnp.where(swap, x, y) for x, y in zip(a, b))
    return low, high


def order_v(x, bits, down, more=above):
    for b in bits:
        for m in range(len(x)):
            if not m >> b & 1:
                x[m], x[m | 1 << b] = order_pair(x[m], x[m | 1 << b], down(m), more)


def order_cross(x, pick, index, bit, down, more):
    other = ~bit
    for m in range(len(x)):
        d = down(m)
        wants = bit if d is False else other if d is True else bit ^ d
        c, k = x[m]
        pc, pk = pick(c, index), pick(k, index)
        if more is above:
            swap = above((c, k), (pc, pk)) ^ wants
        else:
            turn = jnp.where(wants, -1, 0)
            swap = (c ^ turn) > (pc ^ turn)
        x[m] = jnp.where(swap, pc, c), jnp.where(swap, pk, k)


def order_s(x, bits, down, more=above):
    for i in bits:
        order_cross(x, sub_pick, subs() ^ (1 << i), sub_bit(i), down, more)


def order_l(x, bits, down, more=above):
    for i in bits:
        order_cross(x, lane_pick, lanes() ^ (1 << i), lane_bit(i), down, more)


def move_pair(a, b, bit):
    mask = SIGN | np.int32(1 << bit)
    ma, mb = a[0] & mask, b[0] & mask
    a0, b0 = ma == SIGN, mb == SIGN
    a1, b1 = ma == mask, mb == mask
    low = (jnp.where(b0, b[0], jnp.where(a0, a[0], 0)), jnp.where(b0, b[1], a[1]))
    high = (jnp.where(a1, a[0], jnp.where(b1, b[0], 0)), jnp.where(a1, a[1], b[1]))
    return low, high


def move_v(x, steps):
    for bit, i in steps:
        for m in range(len(x)):
            if not m >> i & 1:
                x[m], x[m | 1 << i] = move_pair(x[m], x[m | 1 << i], 16 + bit)


def move_s(x, steps):
    for bit, i in steps:
        b = 16 + bit
        mask = SIGN | np.int32(1 << b)
        here = SIGN | (((subs() >> i) & 1) << b)
        index = subs() ^ (1 << i)
        for m in range(len(x)):
            w, k = x[m]
            pw, pk = sub_pick(w, index), sub_pick(k, index)
            stay, come = (w & mask) == here, (pw & mask) == here
            x[m] = jnp.where(come, pw, jnp.where(stay, w, 0)), jnp.where(come, pk, k)


def turned(x):
    both = []
    for w in range(2):
        t = jnp.concatenate([p[w] for p in x], axis=0).T
        both.append([t[8 * m : 8 * m + 8] for m in range(16)])
    return list(zip(*both))


def batcher(n):
    pairs = []

    def merge(lo, n, r):
        m = r * 2
        if m < n:
            merge(lo, n, m)
            merge(lo + r, n, m)
            for i in range(lo + r, lo + n - r, m):
                pairs.append((i, i + r))
        else:
            pairs.append((lo, lo + r))

    def sort(lo, n):
        if n > 1:
            m = n // 2
            sort(lo, m)
            sort(lo + m, m)
            merge(lo, n, 1)

    sort(0, n)
    return pairs


def total(x):
    s = jnp.sum(x.astype(jnp.float32), axis=0, keepdims=True)
    s = jnp.sum(s, axis=1, keepdims=True)
    return jnp.broadcast_to(s, (8, 128)).astype(jnp.int32)


def sub_prefix(x):
    before, block = jnp.zeros_like(x), x
    for i in range(3):
        other = sub_pick(block, subs() ^ (1 << i))
        before = before + jnp.where(sub_bit(i), other, 0)
        block = block + other
    return before, block


def lane_prefix(x, order, places):
    row = lax.broadcasted_iota(jnp.int32, (128, 128), 0)
    column = lax.broadcasted_iota(jnp.int32, (128, 128), 1)
    x = x.astype(jnp.float32)
    before = [jnp.where(order(row) < place(column), 1.0, 0.0).astype(jnp.float32) for place in places]
    return [total_of(x, m).astype(jnp.int32) for m in before + [jnp.ones((128, 128), jnp.float32)]]


def load(A, B, at):
    return [(A[at + m], B[at + m]) for m in range(16)]


def save(A, B, at, x):
    for m in range(16):
        A[at + m] = x[m][0]
        B[at + m] = x[m][1]


def sort_events(cell, vehicle, speed, A, B):
    flip = -(subs() & 1)
    for block in (0, 16):
        x = []
        for m in range(16):
            c = cell[block + m]
            c = (c & 0x7FF80) | ((c & 7) << 4) | ((c >> 3) & 15)
            level = (speed[block + m] * 1024.0).astype(jnp.int32)
            w = ((c << 13) | (level >> 4)) ^ SIGN
            x.append((w ^ flip, ((level & 15) << 10) | (1023 - vehicle[block + m])))
        for i, j in batcher(16):
            x[i], x[j] = order_pair(x[i], x[j], False, over)
        x = [(w ^ flip, k) for w, k in x]
        for top in (1, 2, 3):
            way = sub_bit(top) if top < 3 else lane_bit(0)
            order_s(x, reversed(range(top)), lambda m: way, over)
            order_v(x, (3, 2, 1, 0), lambda m: way, over)
        save(A, B, block, x)
    for s in range(8, 16):
        if s > 10:
            for block in (0, 16):
                x = turned(load(A, B, block))
                order_v(x, reversed(range(s - 11)), lambda m: bool(m >> (s - 11) & 1), over)
                save(A, B, block, x)
            for m in range(16):
                pair = [(A[m], B[m]), (A[m + 16], B[m + 16])]
                order_v(pair, (0,), lambda _: bool(m >> (s - 11) & 1), over)
                for h in range(2):
                    A[m + 16 * h] = pair[h][0]
                    B[m + 16 * h] = pair[h][1]
        for block in (0, 16):
            x = load(A, B, block)
            way = lane_bit(s - 7) if s < 10 else block > 0 if s == 10 else lane_bit(s - 8) if s < 15 else False
            if s > 9:
                x = turned(x) if s == 10 else x
                order_s(x, (2, 1, 0), lambda m: way if s == 10 else bool(m >> (s - 11) & 1), over)
                x = turned(x)
            else:
                order_l(x, reversed(range(s - 7)), lambda m: way, over)
            order_s(x, (2, 1, 0), lambda m: way, over)
            order_v(x, (3, 2, 1, 0), lambda m: way, over)
            save(A, B, block, x)


def compact_events(A, B):
    lane, sub = lanes(), subs()
    first_edge = (lane & 7) == 0
    lows, ends, blocks = [], [], []
    for block in (0, 16):
        x = load(A, B, block)
        low = [x[0][1]]
        for m in range(1, 16):
            low.append(jnp.where(x[m][0] == x[m - 1][0], jnp.maximum(x[m][1], low[-1]), x[m][1]))
        blocks.append([w for w, _ in x])
        lows.append(low)
        ends.append((pltpu.roll(x[15][0], 1, 0), pltpu.roll(low[15], 1, 0)))
    beside = [tuple(pltpu.roll(t, 1, 1) for t in e) for e in ends]
    across = [beside[1], tuple(pltpu.roll(t, 121, 1) for t in ends[0])]
    flag = jnp.zeros((8, 128), jnp.int32)
    for h in range(2):
        w_before, k_before = (
            jnp.where(sub == 0, jnp.where(first_edge, far, near), own) for far, near, own in zip(across[h], beside[h], ends[h])
        )
        w = blocks[h]
        goes_on = w[0] == w_before
        flag = flag | (goes_on & (w[0] == w[15])).astype(jnp.int32)
        carry = jnp.where(goes_on, k_before, 0)
        lows[h] = [jnp.where(w[m] == w[0], jnp.maximum(lows[h][m], carry), lows[h][m]) for m in range(16)]
    cells = [[((w ^ SIGN) >> 13) & 0x7FFFF for w in blocks[h]] for h in range(2)]
    heads = [pltpu.roll(cells[h][0], 7, 0) for h in range(2)]
    nexts = [pltpu.roll(x, 127, 1) for x in heads]
    edge = (lane & 7) == 7
    follows = [
        jnp.where(sub == 7, jnp.where(edge, pltpu.roll(heads[1], 7, 1), nexts[0]), heads[0]),
        jnp.where(sub == 7, jnp.where(edge, nexts[0], nexts[1]), heads[1]),
    ]
    sums, keeps = [], []
    for h in range(2):
        run = jnp.zeros((8, 128), jnp.int32)
        x = []
        for m in range(16):
            c = cells[h][m]
            keep = c != (cells[h][m + 1] if m < 15 else follows[h])
            if h * 16 + m == 31:
                keep = keep | ((sub == 7) & (lane == 127))
            keeps.append(keep)
            key = ((blocks[h][m] & 0x1FFF) << 14) | lows[h][m] | ((c >> 16) << 27)
            x.append((jnp.where(keep, SIGN | (run << 16) | (c & 0xFFFF), 0), key))
            run = run + keep.astype(jnp.int32)
        save(A, B, 16 * h, x)
        sums.append(sub_prefix(run))
    orders = [lambda l: ((l >> 3) << 4) + (l & 7), lambda l: ((l >> 3) << 4) + (l & 7) + 8]
    parts = [lane_prefix(sums[h][1], orders[h], orders) for h in range(2)]
    every = parts[0][2] + parts[1][2]
    starts = group_starts(cells[0] + cells[1], keeps, every, 16)
    for h in range(2):
        ahead = (parts[0][h] + parts[1][h] + sums[h][0]) << 16
        x = [(jnp.where(w < 0, w + ahead, 0), k) for w, k in load(A, B, 16 * h)]
        move_v(x, [(i, i) for i in range(4)])
        move_s(x, [(4 + i, i) for i in range(3)])
        x = turned(x)
        move_s(x, [(7 + i, i) for i in range(3)])
        save(A, B, 16 * h, x)
    for m in range(16):
        pair = move_pair((A[m], B[m]), (A[m + 16], B[m + 16]), 16 + 10)
        for h in range(2):
            A[m + 16 * h] = pair[h][0]
            B[m + 16 * h] = pair[h][1]
    y = []
    for h in range(2):
        x = load(A, B, 16 * h)
        move_v(x, [(11 + i, i) for i in range(4)])
        y += x[:8]
    flag = flag | crowded(starts, CAP) | (every > 8 * CAP).astype(jnp.int32)
    y = aimed([(w, k & 0x7FFFFFF) for w, k in y], [k >> 27 for _, k in y], [w < 0 for w, _ in y], starts, 0xFFFF)
    return y, flag


def list_rank(v):
    lane = lanes()
    return (v & 7) * CAP + ((v >> 3) << 10) + (subs() << 7) + ((lane & 7) << 4) + (lane >> 3)


def group_starts(cells, keeps, every, shift):
    cells = [jnp.where(u, c, CELLS) for c, u in zip(cells, keeps)]
    starts = [jnp.zeros((8, 128), jnp.int32)]
    for j in range(1, 8):
        t = jnp.zeros((8, 128), jnp.int32)
        for c in cells:
            t = t + jnp.where(c < j << shift, 1, 0)
        starts.append(total(t))
    return starts + [every]


def crowded(starts, room):
    most = jnp.zeros((8, 128), jnp.int32)
    for j in range(8):
        most = jnp.maximum(most, starts[j + 1] - starts[j])
    return (most > room).astype(jnp.int32)


def aimed(x, groups, valid, starts, mask):
    made = []
    for v, (w, k) in enumerate(x):
        target = list_rank(v)
        moved = jnp.zeros((8, 128), jnp.int32)
        for j in range(1, 8):
            moved = jnp.where(groups[v] == j, j * CAP - starts[j], moved)
        made.append((jnp.where(valid[v], SIGN | ((target + moved) << 16) | (w & mask), 0), k))
    return made


def expand_lists(x):
    move_v(x, [(13, 2), (12, 1), (11, 0), (10, 3)])
    move_s(x, [(9, 2), (8, 1), (7, 0)])
    x = turned(x)
    move_s(x, [(6, 2), (5, 1), (4, 0)])
    move_v(x, [(3, 3), (2, 2), (1, 1), (0, 0)])
    return turned(x)


def planes(w, k):
    return (
        jnp.where(w < 0, w & 0xFFFF, EMPTY).astype(jnp.float32),
        (k >> 10).astype(jnp.float32) * (1.0 / 1024.0),
        (1023 - (k & 1023)).astype(jnp.float32),
    )


def pack_messages(x, out):
    for v, pair in enumerate(x):
        for p, plane in enumerate(planes(*pair)):
            out[v & 7, 2 * p + (v >> 3)] = plane


def pack_short(x, out):
    for v, pair in enumerate(x):
        for p, plane in enumerate(planes(*pair)):
            if v < 8:
                out[v, 3 * p] = plane[:4]
                out[v, 3 * p + 1] = plane[4:]
            else:
                out[v - 8, 3 * p + 2] = plane[:4]


def key_of(speed, vehicle):
    return (speed * 1024.0).astype(jnp.int32) * 1024 + (1023 - vehicle.astype(jnp.int32))


def merge_lists(inbox):
    around, back = 7 - subs(), 127 - lanes()
    x = [None] * 16
    for s in range(8):
        for h in range(2):
            pair = (inbox[s, h].astype(jnp.int32), key_of(inbox[s, 2 + h], inbox[s, 4 + h]))
            if s & 1:
                x[8 * (1 - h) + s] = tuple(lane_pick(sub_pick(w, around), back) for w in pair)
            else:
                x[8 * h + s] = pair
    for level in (1, 2, 3):
        down = (lambda m: bool(m >> level & 1)) if level < 3 else (lambda m: False)
        way = lane_bit(3 + level) if level < 3 else False
        order_v(x, (*reversed(range(level)), 3), down)
        order_s(x, (2, 1, 0), down)
        x = turned(x)
        order_s(x, (2, 1, 0), lambda m: way)
        order_v(x, (3, 2, 1, 0), lambda m: way)
        if level < 3:
            x = turned(x)
    return x


def best_of_cells(x, tell):
    lane, sub = lanes(), subs()
    head = pltpu.roll(x[0][0], 7, 0)
    beyond = jnp.where(lane < 64, pltpu.roll(head, 71, 1), pltpu.roll(head, 63, 1))
    carried = jnp.where((lane & 7) == 7, beyond, pltpu.roll(head, 127, 1))
    follow = jnp.where(sub == 7, carried, head)
    run = jnp.zeros((8, 128), jnp.int32)
    y, keeps = [], []
    for m in range(16):
        c, k = x[m]
        keep = c != (x[m + 1][0] if m < 15 else follow)
        if m == 15:
            keep = keep | ((sub == 7) & (lane == 127))
        keep = keep & (c < EMPTY)
        keeps.append(keep)
        y.append((jnp.where(keep, SIGN | (run << 16) | c, 0), k))
        run = run + keep.astype(jnp.int32)
    within, block = sub_prefix(run)
    order = lambda l: (((l >> 3) & 7) << 4) + ((l >> 6) << 3) + (l & 7)
    ahead, every = lane_prefix(block, order, [order])
    starts = group_starts([c for c, _ in x], keeps, every, 13)
    tell(crowded(starts, SHORT))
    start = (within + ahead) << 16
    y = [(jnp.where(w < 0, w + start, 0), k) for w, k in y]
    move_v(y, [(i, i) for i in range(4)])
    move_s(y, [(4 + i, i) for i in range(3)])
    y = turned(y)
    move_s(y, [(7 + i, i) for i in range(3)])
    move_v(y, [(10, 3), (11, 0), (12, 1), (13, 2)])
    return y, starts


def regroup(x, tell):
    y, starts = best_of_cells(x, tell)
    groups = [(w >> 13) & 7 for w, _ in y]
    valid = [w < 0 for w, _ in y]
    return expand_lists(aimed(y, groups, valid, starts, 0x1FFF))


def short_list(inbox, s):
    made = []
    for h in range(2):
        low, high = (3 * h, 1) if h == 0 else (2, 2)
        c, speed, vehicle = (
            jnp.concatenate([inbox[s, 3 * p + low], inbox[s, 3 * p + high]], axis=0) for p in range(3)
        )
        used = c < EMPTY
        if h:
            used = used & (subs() < 4)
        made.append((jnp.where(used, SIGN | (c.astype(jnp.int32) << 16), 0), key_of(speed, vehicle)))
    return made


def spread_lists(inbox, pair):
    x = []
    mask = SIGN | np.int32(3 << 27)
    for s in pair:
        words = short_list(inbox, s)
        for high in range(4):
            mine = SIGN | np.int32(high << 27)
            some = [(jnp.where((w & mask) == mine, w, 0), k) for w, k in words]
            move_v(some, [(10, 0)])
            x += some
    move_s(x, [(9, 2), (8, 1), (7, 0)])
    x = turned(x)
    move_s(x, [(6, 2), (5, 1), (4, 0)])
    move_v(x, [(3, 3), (2, 2), (1, 1), (0, 0)])
    return [jnp.where(w < 0, k, -1) for w, k in x]


def joined(tables):
    best = tables[0]
    for t in tables[1:]:
        best = [jnp.maximum(a, b) for a, b in zip(best, t)]
    t = jnp.concatenate(best, axis=0).T
    return [jnp.maximum(t[8 * z : 8 * z + 8], t[64 + 8 * z : 72 + 8 * z]) for z in range(8)]


def exchange_kernel(cell, vehicle, speed, both, flags, events, reals, A, B, out1, in1, out2, in2, out3, in3, mark, plane,
                    marks, arrive, send, recv, plane_send, plane_recv):
    gx, gy = lax.axis_index("gx"), lax.axis_index("gy")
    y, z = gy // 8, gy % 8
    loads = [
        pltpu.make_async_copy(cell, events.at[0], arrive.at[0]),
        pltpu.make_async_copy(vehicle, events.at[1], arrive.at[1]),
        pltpu.make_async_copy(speed, reals, arrive.at[2]),
    ]
    for c in loads:
        c.start()

    def peer(phase, j):
        if phase == 0:
            return (gx ^ j, gy)
        if phase == 1:
            return (gx, (y ^ j) * 8 + z)
        return (gx, y * 8 + (z ^ j))

    def in_plane(j):
        return (gx ^ (j & 7), y * 8 + (z ^ (j >> 3)))

    barrier = pltpu.get_barrier_semaphore()
    for j in range(1, 8):
        pl.semaphore_signal(barrier, inc=1, device_id=peer(1, j), device_id_type=MESH)

    def greet(j, _):
        pl.semaphore_signal(barrier, inc=1, device_id=in_plane(j), device_id_type=MESH)
        return 0

    lax.fori_loop(1, 64, greet, 0)

    def copies(row, phase, source, target):
        return [
            pltpu.make_async_remote_copy(
                src_ref=source(j),
                dst_ref=target(j),
                send_sem=send.at[row, j],
                recv_sem=recv.at[row, j],
                device_id=peer(phase, j),
                device_id_type=MESH,
            )
            for j in FAR_FIRST[phase]
        ]

    def to_plane(j):
        return pltpu.make_async_remote_copy(
            src_ref=plane.at[0],
            dst_ref=plane.at[j],
            send_sem=plane_send.at[j],
            recv_sem=plane_recv.at[j],
            device_id=in_plane(j),
            device_id_type=MESH,
        )

    def over_plane(act):
        def step(j, _):
            act(to_plane(j))
            return 0

        lax.fori_loop(1, 64, step, 0)

    for c in loads:
        c.wait()
    sort_events(events.at[0], events.at[1], reals, A, B)
    x, flag = compact_events(A, B)
    pack_messages(expand_lists(x), out1)
    pl.semaphore_wait(barrier, 70)
    first = copies(0, 0, lambda j: out1.at[gx ^ j], lambda j: in1.at[j])
    for c in first:
        c.start()
    in1[0] = out1[gx]
    for c in first:
        c.wait_recv()

    def tell(more):
        plane[0] = jnp.max((flag | more).astype(jnp.float32), axis=0, keepdims=True)

    x = regroup(merge_lists(in1), tell)
    pack_short(x, out2)
    second = copies(1, 1, lambda j: out2.at[y ^ j], lambda j: in2.at[j])
    for c in second:
        c.start()
    in2[0] = out2[y]
    over_plane(lambda c: c.start())

    tables = []
    for pair in ((0, 1), (2, 6), (3, 7), (4, 5)):
        for j in pair:
            if j:
                second[FAR_FIRST[1].index(j)].wait_recv()
        tables.append(spread_lists(in2, pair))
    for v, k in enumerate(joined(tables)):
        there = k >= 0
        out3[v, 0] = jnp.where(there, (k >> 10).astype(jnp.float32) * (1.0 / 1024.0), -1.0)
        out3[v, 1] = jnp.where(there, (1023 - (k & 1023)).astype(jnp.float32), 1024.0)
    third = copies(2, 2, lambda j: out3.at[z ^ j], lambda j: in3.at[j])
    for c in third:
        c.start()
    in3[0] = out3[z]
    over_plane(lambda c: c.wait_recv())
    mark[...] = jnp.max(plane[...], axis=0)
    told = copies(3, 1, lambda j: mark, lambda j: marks.at[j])
    for c in told:
        c.start()
    k = key_of(in3[0, 0], in3[0, 1])
    for j in reversed(FAR_FIRST[2]):
        third[FAR_FIRST[2].index(j)].wait_recv()
        k = jnp.maximum(k, key_of(in3[j, 0], in3[j, 1]))
    both[0] = jnp.where(k < 0, -1.0, (k >> 10).astype(jnp.float32) * (1.0 / 1024.0))
    both[1] = jnp.where(k < 0, -1, 1023 - (k & 1023)).astype(jnp.float32)
    seen = mark[...]
    for c in told:
        c.wait_recv()
    for j in range(1, 8):
        seen = jnp.maximum(seen, marks[j])
    flags[0, 0] = jnp.max(seen).astype(jnp.int32)
    for group in (first, second, third, told):
        for c in group:
            c.wait_send()
    over_plane(lambda c: c.wait_send())


def words(*shape):
    return pltpu.VMEM(shape + (8, 128), jnp.float32)


def sparse_path(cell, vehicle, speed):
    whole = pl.BlockSpec(memory_space=pltpu.VMEM)
    ints = lambda n: pltpu.VMEM((n, 8, 128), jnp.int32)
    return pl.pallas_call(
        exchange_kernel,
        out_shape=(
            jax.ShapeDtypeStruct((2, 8, 128), jnp.float32),
            jax.ShapeDtypeStruct((1, 1), jnp.int32),
        ),
        in_specs=[pl.BlockSpec(memory_space=pl.ANY)] * 3,
        out_specs=(whole, pl.BlockSpec(memory_space=pltpu.SMEM)),
        scratch_shapes=[
            pltpu.VMEM((2, 32, 8, 128), jnp.int32),
            words(32),
            ints(32),
            ints(32),
            words(8, 6),
            words(8, 6),
            pltpu.VMEM((8, 9, 4, 128), jnp.float32),
            pltpu.VMEM((8, 9, 4, 128), jnp.float32),
            words(8, 2),
            words(8, 2),
            pltpu.VMEM((1, 128), jnp.float32),
            pltpu.VMEM((64, 1, 128), jnp.float32),
            pltpu.VMEM((8, 1, 128), jnp.float32),
            pltpu.SemaphoreType.DMA((3,)),
            pltpu.SemaphoreType.DMA((4, 8)),
            pltpu.SemaphoreType.DMA((4, 8)),
            pltpu.SemaphoreType.DMA((64,)),
            pltpu.SemaphoreType.DMA((64,)),
        ],
        compiler_params=pltpu.CompilerParams(collective_id=0, has_side_effects=True),
    )(cell, vehicle, speed)


def per_device(cell, vehicle, speed):
    shaped = [x.reshape(32, 8, 128) for x in (cell, vehicle, speed)]
    both, flags = sparse_path(*shaped)
    both = lax.cond(flags[0, 0] > 0, lambda: dense_path(cell, vehicle, speed), lambda: both)
    return both[0].reshape(1024), both[1].astype(jnp.int32).reshape(1024)


def solution(mesh):
    placed = (P(("gx", "gy")), P(("gx", "gy")), P(("gx", "gy")))
    return jax.shard_map(
        per_device,
        mesh=mesh,
        in_specs=placed,
        out_specs=(P(("gx", "gy")), P(("gx", "gy"))),
        check_vma=False,
    )
```

```python
import jax
import jax.numpy as jnp
import numpy as np
from jax import lax
from jax.experimental import pallas as pl
from jax.experimental.pallas import tpu as pltpu
from jax.sharding import PartitionSpec as P

CELLS = 524288
VEHICLES = 1024
MESH = pl.DeviceIdType.MESH
FAR_FIRST = ((4, 5, 6, 7, 2, 3, 1), (4, 5, 3, 7, 6, 2, 1), (4, 5, 3, 7, 6, 2, 1))
SIGN = np.int32(-(2**31))
CAP = 2048
SHORT = 1536
EMPTY = 131072


def swapped(block, axis, apart):
    count = lax.axis_size(axis)
    route = []
    for low in range(count):
        high = low | 1 << apart
        if high != low and high < count:
            route += [(low, high), (high, low)]
    return lax.ppermute(block, axis, route)


def combine(first, second):
    speed_a = first[0]
    speed_b = second[0]
    best = jnp.maximum(speed_a, speed_b)
    ident = jnp.where(
        speed_a > speed_b,
        first[1],
        jnp.where(speed_b > speed_a, second[1], jnp.minimum(first[1], second[1])),
    )
    return jnp.stack([best, ident])


def dense_path(cell, vehicle, speed):
    local_best = jnp.full((CELLS,), -1.0, jnp.float32).at[cell].max(speed)
    chosen = jnp.where(speed == local_best[cell], vehicle, VEHICLES)
    local_ident = jnp.full((CELLS,), VEHICLES, jnp.int32).at[cell].min(chosen)
    paired = jnp.stack([local_best, local_ident.astype(jnp.float32)])
    outer = lax.axis_size("gx")
    inner = lax.axis_size("gy")
    nbits = (outer * inner).bit_length() - 1
    myself = lax.axis_index(("gx", "gy"))
    buffer = paired
    for level in reversed(range(nbits)):
        half = buffer.shape[1] // 2
        side = myself >> level & 1
        keep = lax.dynamic_slice_in_dim(buffer, side * half, half, 1)
        give = lax.dynamic_slice_in_dim(buffer, (1 - side) * half, half, 1)
        partner = swapped(give, ("gx", "gy"), level)
        buffer = combine(keep, partner)
    best = buffer[0]
    lowest = buffer[1].astype(jnp.int32)
    top_vehicle = jnp.where(lowest < VEHICLES, lowest, -1)
    return jnp.stack([best, top_vehicle.astype(jnp.float32)]).reshape(2, 8, 128)


def lanes():
    return lax.broadcasted_iota(jnp.int32, (8, 128), 1)


def subs():
    return lax.broadcasted_iota(jnp.int32, (8, 128), 0)


def lane_pick(x, index):
    return jnp.take_along_axis(x, index, axis=1)


def sub_pick(x, index):
    return jnp.take_along_axis(x, index, axis=0)


def sub_bit(i):
    return ((subs() >> i) & 1) == 1


def lane_bit(i):
    return ((lanes() >> i) & 1) == 1


def total_of(counts, matrix):
    return jnp.dot(counts, matrix, preferred_element_type=jnp.float32)


def above(x, y):
    tie = x[0] == y[0]
    return jnp.where(tie, x[1], x[0]) > jnp.where(tie, y[1], y[0])


def over(x, y):
    return x[0] > y[0]


def order_pair(a, b, down, more=above):
    swap = more(a, b)
    if down is True:
        a, b = b, a
    elif down is not False:
        swap = swap ^ down
    low = tuple(jnp.where(swap, y, x) for x, y in zip(a, b))
    high = tuple(jnp.where(swap, x, y) for x, y in zip(a, b))
    return low, high


def order_v(x, bits, down, more=above):
    for b in bits:
        for m in range(len(x)):
            if not m >> b & 1:
                x[m], x[m | 1 << b] = order_pair(x[m], x[m | 1 << b], down(m), more)


def order_cross(x, pick, index, bit, down, more):
    other = ~bit
    for m in range(len(x)):
        d = down(m)
        wants = bit if d is False else other if d is True else bit ^ d
        c, k = x[m]
        pc, pk = pick(c, index), pick(k, index)
        if more is above:
            swap = above((c, k), (pc, pk)) ^ wants
        else:
            turn = jnp.where(wants, -1, 0)
            swap = (c ^ turn) > (pc ^ turn)
        x[m] = jnp.where(swap, pc, c), jnp.where(swap, pk, k)


def order_s(x, bits, down, more=above):
    for i in bits:
        order_cross(x, sub_pick, subs() ^ (1 << i), sub_bit(i), down, more)


def order_l(x, bits, down, more=above):
    for i in bits:
        order_cross(x, lane_pick, lanes() ^ (1 << i), lane_bit(i), down, more)


def move_pair(a, b, bit):
    mask = SIGN | np.int32(1 << bit)
    ma, mb = a[0] & mask, b[0] & mask
    a0, b0 = ma == SIGN, mb == SIGN
    a1, b1 = ma == mask, mb == mask
    low = (jnp.where(b0, b[0], jnp.where(a0, a[0], 0)), jnp.where(b0, b[1], a[1]))
    high = (jnp.where(a1, a[0], jnp.where(b1, b[0], 0)), jnp.where(a1, a[1], b[1]))
    return low, high


def move_v(x, steps):
    for bit, i in steps:
        for m in range(len(x)):
            if not m >> i & 1:
                x[m], x[m | 1 << i] = move_pair(x[m], x[m | 1 << i], 16 + bit)


def move_s(x, steps):
    for bit, i in steps:
        b = 16 + bit
        mask = SIGN | np.int32(1 << b)
        here = SIGN | (((subs() >> i) & 1) << b)
        index = subs() ^ (1 << i)
        for m in range(len(x)):
            w, k = x[m]
            pw, pk = sub_pick(w, index), sub_pick(k, index)
            stay, come = (w & mask) == here, (pw & mask) == here
            x[m] = jnp.where(come, pw, jnp.where(stay, w, 0)), jnp.where(come, pk, k)


def turned(x):
    both = []
    for w in range(2):
        t = jnp.concatenate([p[w] for p in x], axis=0).T
        both.append([t[8 * m : 8 * m + 8] for m in range(16)])
    return list(zip(*both))


def batcher(n):
    pairs = []

    def merge(lo, n, r):
        m = r * 2
        if m < n:
            merge(lo, n, m)
            merge(lo + r, n, m)
            for i in range(lo + r, lo + n - r, m):
                pairs.append((i, i + r))
        else:
            pairs.append((lo, lo + r))

    def sort(lo, n):
        if n > 1:
            m = n // 2
            sort(lo, m)
            sort(lo + m, m)
            merge(lo, n, 1)

    sort(0, n)
    return pairs


def total(x):
    s = jnp.sum(x.astype(jnp.float32), axis=0, keepdims=True)
    s = jnp.sum(s, axis=1, keepdims=True)
    return jnp.broadcast_to(s, (8, 128)).astype(jnp.int32)


def sub_prefix(x):
    before, block = jnp.zeros_like(x), x
    for i in range(3):
        other = sub_pick(block, subs() ^ (1 << i))
        before = before + jnp.where(sub_bit(i), other, 0)
        block = block + other
    return before, block


def lane_prefix(x, order, places):
    row = lax.broadcasted_iota(jnp.int32, (128, 128), 0)
    column = lax.broadcasted_iota(jnp.int32, (128, 128), 1)
    x = x.astype(jnp.float32)
    before = [jnp.where(order(row) < place(column), 1.0, 0.0).astype(jnp.float32) for place in places]
    return [total_of(x, m).astype(jnp.int32) for m in before + [jnp.ones((128, 128), jnp.float32)]]


def load(A, B, at):
    return [(A[at + m], B[at + m]) for m in range(16)]


def save(A, B, at, x):
    for m in range(16):
        A[at + m] = x[m][0]
        B[at + m] = x[m][1]


def sort_events(cell, vehicle, speed, A, B):
    flip = -(subs() & 1)
    for block in (0, 16):
        x = []
        for m in range(16):
            c = cell[block + m]
            c = (c & 0x7FF80) | ((c & 7) << 4) | ((c >> 3) & 15)
            level = (speed[block + m] * 1024.0).astype(jnp.int32)
            w = ((c << 13) | (level >> 4)) ^ SIGN
            x.append((w ^ flip, ((level & 15) << 10) | (1023 - vehicle[block + m])))
        for i, j in batcher(16):
            x[i], x[j] = order_pair(x[i], x[j], False, over)
        x = [(w ^ flip, k) for w, k in x]
        for top in (1, 2, 3):
            way = sub_bit(top) if top < 3 else lane_bit(0)
            order_s(x, reversed(range(top)), lambda m: way, over)
            order_v(x, (3, 2, 1, 0), lambda m: way, over)
        save(A, B, block, x)
    for s in range(8, 16):
        if s > 10:
            for block in (0, 16):
                x = turned(load(A, B, block))
                order_v(x, reversed(range(s - 11)), lambda m: bool(m >> (s - 11) & 1), over)
                save(A, B, block, x)
            for m in range(16):
                pair = [(A[m], B[m]), (A[m + 16], B[m + 16])]
                order_v(pair, (0,), lambda _: bool(m >> (s - 11) & 1), over)
                for h in range(2):
                    A[m + 16 * h] = pair[h][0]
                    B[m + 16 * h] = pair[h][1]
        for block in (0, 16):
            x = load(A, B, block)
            way = lane_bit(s - 7) if s < 10 else block > 0 if s == 10 else lane_bit(s - 8) if s < 15 else False
            if s > 9:
                x = turned(x) if s == 10 else x
                order_s(x, (2, 1, 0), lambda m: way if s == 10 else bool(m >> (s - 11) & 1), over)
                x = turned(x)
            else:
                order_l(x, reversed(range(s - 7)), lambda m: way, over)
            order_s(x, (2, 1, 0), lambda m: way, over)
            order_v(x, (3, 2, 1, 0), lambda m: way, over)
            save(A, B, block, x)


def compact_events(A, B, me):
    lane, sub = lanes(), subs()
    first_edge = (lane & 7) == 0
    lows, ends, blocks = [], [], []
    for block in (0, 16):
        x = load(A, B, block)
        low = [x[0][1]]
        for m in range(1, 16):
            low.append(jnp.where(x[m][0] == x[m - 1][0], jnp.maximum(x[m][1], low[-1]), x[m][1]))
        blocks.append([w for w, _ in x])
        lows.append(low)
        ends.append((pltpu.roll(x[15][0], 1, 0), pltpu.roll(low[15], 1, 0)))
    beside = [tuple(pltpu.roll(t, 1, 1) for t in e) for e in ends]
    across = [beside[1], tuple(pltpu.roll(t, 121, 1) for t in ends[0])]
    flag = jnp.zeros((8, 128), jnp.int32)
    for h in range(2):
        w_before, k_before = (
            jnp.where(sub == 0, jnp.where(first_edge, far, near), own) for far, near, own in zip(across[h], beside[h], ends[h])
        )
        w = blocks[h]
        goes_on = w[0] == w_before
        flag = flag | (goes_on & (w[0] == w[15])).astype(jnp.int32)
        carry = jnp.where(goes_on, k_before, 0)
        lows[h] = [jnp.where(w[m] == w[0], jnp.maximum(lows[h][m], carry), lows[h][m]) for m in range(16)]
    cells = [[((w ^ SIGN) >> 13) & 0x7FFFF for w in blocks[h]] for h in range(2)]
    heads = [pltpu.roll(cells[h][0], 7, 0) for h in range(2)]
    nexts = [pltpu.roll(x, 127, 1) for x in heads]
    edge = (lane & 7) == 7
    follows = [
        jnp.where(sub == 7, jnp.where(edge, pltpu.roll(heads[1], 7, 1), nexts[0]), heads[0]),
        jnp.where(sub == 7, jnp.where(edge, nexts[0], nexts[1]), heads[1]),
    ]
    sums, keeps = [], []
    for h in range(2):
        run = jnp.zeros((8, 128), jnp.int32)
        x = []
        for m in range(16):
            c = cells[h][m]
            keep = c != (cells[h][m + 1] if m < 15 else follows[h])
            if h * 16 + m == 31:
                keep = keep | ((sub == 7) & (lane == 127))
            keeps.append(keep)
            key = ((blocks[h][m] & 0x1FFF) << 14) | lows[h][m] | ((c >> 16) << 27)
            x.append((jnp.where(keep, SIGN | (run << 16) | (c & 0xFFFF), 0), key))
            run = run + keep.astype(jnp.int32)
        save(A, B, 16 * h, x)
        sums.append(sub_prefix(run))
    orders = [lambda l: ((l >> 3) << 4) + (l & 7), lambda l: ((l >> 3) << 4) + (l & 7) + 8]
    parts = [lane_prefix(sums[h][1], orders[h], orders) for h in range(2)]
    every = parts[0][2] + parts[1][2]
    starts = group_starts(cells[0] + cells[1], keeps, every, 16)
    for h in range(2):
        ahead = (parts[0][h] + parts[1][h] + sums[h][0]) << 16
        x = [(jnp.where(w < 0, w + ahead, 0), k) for w, k in load(A, B, 16 * h)]
        move_v(x, [(i, i) for i in range(4)])
        move_s(x, [(4 + i, i) for i in range(3)])
        x = turned(x)
        move_s(x, [(7 + i, i) for i in range(3)])
        save(A, B, 16 * h, x)
    for m in range(16):
        pair = move_pair((A[m], B[m]), (A[m + 16], B[m + 16]), 16 + 10)
        for h in range(2):
            A[m + 16 * h] = pair[h][0]
            B[m + 16 * h] = pair[h][1]
    y = []
    for h in range(2):
        x = load(A, B, 16 * h)
        move_v(x, [(11 + i, i) for i in range(4)])
        y += x[:8]
    flag = flag | crowded(starts, CAP) | (every > 8 * CAP).astype(jnp.int32)
    y = aimed([(w, k & 0x7FFFFFF) for w, k in y], [k >> 27 for _, k in y], [w < 0 for w, _ in y], starts, 0xFFFF, me)
    return y, flag


def list_rank(v):
    lane = lanes()
    return (v & 7) * CAP + ((v >> 3) << 10) + (subs() << 7) + ((lane & 7) << 4) + (lane >> 3)


def group_starts(cells, keeps, every, shift):
    cells = [jnp.where(u, c, CELLS) for c, u in zip(cells, keeps)]
    starts = [jnp.zeros((8, 128), jnp.int32)]
    for j in range(1, 8):
        t = jnp.zeros((8, 128), jnp.int32)
        for c in cells:
            t = t + jnp.where(c < j << shift, 1, 0)
        starts.append(total(t))
    return starts + [every]


def crowded(starts, room):
    most = jnp.zeros((8, 128), jnp.int32)
    for j in range(8):
        most = jnp.maximum(most, starts[j + 1] - starts[j])
    return (most > room).astype(jnp.int32)


def aimed(x, groups, valid, starts, mask, me=None):
    made = []
    for v, (w, k) in enumerate(x):
        target = list_rank(v)
        moved = jnp.zeros((8, 128), jnp.int32)
        for j in range(1, 8):
            moved = jnp.where(groups[v] == j, j * CAP - starts[j], moved)
        target = target + moved
        if me is not None:
            target = target ^ (-((groups[v] ^ me) & 1) & (CAP - 1))
        made.append((jnp.where(valid[v], SIGN | (target << 16) | (w & mask), 0), k))
    return made


def expand_lists(x):
    move_v(x, [(13, 2), (12, 1), (11, 0), (10, 3)])
    move_s(x, [(9, 2), (8, 1), (7, 0)])
    x = turned(x)
    move_s(x, [(6, 2), (5, 1), (4, 0)])
    move_v(x, [(3, 3), (2, 2), (1, 1), (0, 0)])
    return turned(x)


def planes(w, k):
    return (
        jnp.where(w < 0, w & 0xFFFF, EMPTY).astype(jnp.float32),
        (k >> 10).astype(jnp.float32) * (1.0 / 1024.0),
        (1023 - (k & 1023)).astype(jnp.float32),
    )


def pack_messages(x, out):
    for v, pair in enumerate(x):
        for p, plane in enumerate(planes(*pair)):
            out[v & 7, 2 * p + (v >> 3)] = plane


def pack_short(x, out):
    for v, pair in enumerate(x):
        for p, plane in enumerate(planes(*pair)):
            if v < 8:
                out[v, 3 * p] = plane[:4]
                out[v, 3 * p + 1] = plane[4:]
            else:
                out[v - 8, 3 * p + 2] = plane[:4]


def key_of(speed, vehicle):
    return (speed * 1024.0).astype(jnp.int32) * 1024 + (1023 - vehicle.astype(jnp.int32))


def merge_lists(inbox):
    x = [(inbox[s, h].astype(jnp.int32), key_of(inbox[s, 2 + h], inbox[s, 4 + h])) for h in range(2) for s in range(8)]
    for level in (1, 2, 3):
        down = (lambda m: bool(m >> level & 1)) if level < 3 else (lambda m: False)
        way = lane_bit(3 + level) if level < 3 else False
        order_v(x, (*reversed(range(level)), 3), down, over)
        order_s(x, (2, 1, 0), down, over)
        x = turned(x)
        order_s(x, (2, 1, 0), lambda m: way, over)
        order_v(x, (3, 2, 1, 0), lambda m: way, over)
        if level < 3:
            x = turned(x)
    return x


def best_of_cells(x, tell):
    lane, sub = lanes(), subs()
    head = pltpu.roll(x[0][0], 7, 0)
    beyond = jnp.where(lane < 64, pltpu.roll(head, 71, 1), pltpu.roll(head, 63, 1))
    carried = jnp.where((lane & 7) == 7, beyond, pltpu.roll(head, 127, 1))
    follow = jnp.where(sub == 7, carried, head)
    keys = [x[0][1]]
    for m in range(1, 16):
        keys.append(jnp.where(x[m][0] == x[m - 1][0], jnp.maximum(x[m][1], keys[-1]), x[m][1]))
    before = []
    for t in (pltpu.roll(x[15][0], 1, 0), pltpu.roll(keys[15], 1, 0)):
        far = jnp.where(lane < 64, pltpu.roll(t, 65, 1), pltpu.roll(t, 57, 1))
        before.append(jnp.where(sub == 0, jnp.where((lane & 7) == 0, far, pltpu.roll(t, 1, 1)), t))
    carry = jnp.where(x[0][0] == before[0], before[1], 0)
    run = jnp.zeros((8, 128), jnp.int32)
    y, keeps = [], []
    for m in range(16):
        c = x[m][0]
        k = jnp.where(c == x[0][0], jnp.maximum(keys[m], carry), keys[m])
        keep = c != (x[m + 1][0] if m < 15 else follow)
        if m == 15:
            keep = keep | ((sub == 7) & (lane == 127))
        keep = keep & (c < EMPTY)
        keeps.append(keep)
        y.append((jnp.where(keep, SIGN | (run << 16) | c, 0), k))
        run = run + keep.astype(jnp.int32)
    within, block = sub_prefix(run)
    order = lambda l: (((l >> 3) & 7) << 4) + ((l >> 6) << 3) + (l & 7)
    ahead, every = lane_prefix(block, order, [order])
    starts = group_starts([c for c, _ in x], keeps, every, 13)
    tell(crowded(starts, SHORT))
    start = (within + ahead) << 16
    y = [(jnp.where(w < 0, w + start, 0), k) for w, k in y]
    move_v(y, [(i, i) for i in range(4)])
    move_s(y, [(4 + i, i) for i in range(3)])
    y = turned(y)
    move_s(y, [(7 + i, i) for i in range(3)])
    move_v(y, [(10, 3), (11, 0), (12, 1), (13, 2)])
    return y, starts


def regroup(x, tell):
    y, starts = best_of_cells(x, tell)
    groups = [(w >> 13) & 7 for w, _ in y]
    valid = [w < 0 for w, _ in y]
    return expand_lists(aimed(y, groups, valid, starts, 0x1FFF))


def short_list(inbox, s):
    made = []
    for h in range(2):
        low, high = (3 * h, 1) if h == 0 else (2, 2)
        c, speed, vehicle = (
            jnp.concatenate([inbox[s, 3 * p + low], inbox[s, 3 * p + high]], axis=0) for p in range(3)
        )
        used = c < EMPTY
        if h:
            used = used & (subs() < 4)
        made.append((jnp.where(used, SIGN | (c.astype(jnp.int32) << 16), 0), key_of(speed, vehicle)))
    return made


def spread_lists(inbox, pair):
    x = []
    mask = SIGN | np.int32(3 << 27)
    for s in pair:
        words = short_list(inbox, s)
        for high in range(4):
            mine = SIGN | np.int32(high << 27)
            some = [(jnp.where((w & mask) == mine, w, 0), k) for w, k in words]
            move_v(some, [(10, 0)])
            x += some
    move_s(x, [(9, 2), (8, 1), (7, 0)])
    x = turned(x)
    move_s(x, [(6, 2), (5, 1), (4, 0)])
    move_v(x, [(3, 3), (2, 2), (1, 1), (0, 0)])
    return [jnp.where(w < 0, k, -1) for w, k in x]


def joined(tables):
    best = tables[0]
    for t in tables[1:]:
        best = [jnp.maximum(a, b) for a, b in zip(best, t)]
    t = jnp.concatenate(best, axis=0).T
    return [jnp.maximum(t[8 * z : 8 * z + 8], t[64 + 8 * z : 72 + 8 * z]) for z in range(8)]


def exchange_kernel(cell, vehicle, speed, both, flags, events, reals, A, B, out1, in1, out2, in2, out3, in3, mark, marks,
                    arrive, send, recv):
    gx, gy = lax.axis_index("gx"), lax.axis_index("gy")
    y, z = gy // 8, gy % 8
    loads = [
        pltpu.make_async_copy(cell, events.at[0], arrive.at[0]),
        pltpu.make_async_copy(vehicle, events.at[1], arrive.at[1]),
        pltpu.make_async_copy(speed, reals, arrive.at[2]),
    ]
    for c in loads:
        c.start()

    def peer(phase, j):
        if phase == 0:
            return (gx ^ j, gy)
        if phase == 1:
            return (gx, (y ^ j) * 8 + z)
        return (gx, y * 8 + (z ^ j))

    barrier = pltpu.get_barrier_semaphore()
    for phase in range(3):
        for j in range(1, 8):
            pl.semaphore_signal(barrier, inc=1, device_id=peer(phase, j), device_id_type=MESH)

    def copies(row, phase, source, target):
        return [
            pltpu.make_async_remote_copy(
                src_ref=source(j),
                dst_ref=target(j),
                send_sem=send.at[row, j],
                recv_sem=recv.at[row, j],
                device_id=peer(phase, j),
                device_id_type=MESH,
            )
            for j in FAR_FIRST[phase]
        ]

    def share(phase, seen):
        mark[phase] = seen
        made = copies(3 + phase, phase, lambda j: mark.at[phase], lambda j: marks.at[phase, j])
        for c in made:
            c.start()
        return made

    def seen_by(phase, made, seen):
        for c in made:
            c.wait_recv()
        for j in range(1, 8):
            seen = jnp.maximum(seen, marks[phase, j])
        return seen

    for c in loads:
        c.wait()
    sort_events(events.at[0], events.at[1], reals, A, B)
    x, flag = compact_events(A, B, gx)
    pack_messages(expand_lists(x), out1)
    pl.semaphore_wait(barrier, 21)
    first = copies(0, 0, lambda j: out1.at[gx ^ j], lambda j: in1.at[j])
    for c in first:
        c.start()
    in1[0] = out1[gx]
    for c in first:
        c.wait_recv()

    told = []

    def tell(more):
        seen = jnp.max((flag | more).astype(jnp.float32), axis=0, keepdims=True)
        told.append((share(0, seen), seen))

    x = regroup(merge_lists(in1), tell)
    pack_short(x, out2)
    second = copies(1, 1, lambda j: out2.at[y ^ j], lambda j: in2.at[j])
    for c in second:
        c.start()
    in2[0] = out2[y]
    seen = seen_by(0, *told[0])
    told.append((share(2, seen), seen))

    tables = []
    for pair in ((0, 1), (2, 6), (3, 7), (4, 5)):
        for j in pair:
            if j:
                second[FAR_FIRST[1].index(j)].wait_recv()
        tables.append(spread_lists(in2, pair))
    for v, k in enumerate(joined(tables)):
        there = k >= 0
        out3[v, 0] = jnp.where(there, (k >> 10).astype(jnp.float32) * (1.0 / 1024.0), -1.0)
        out3[v, 1] = jnp.where(there, (1023 - (k & 1023)).astype(jnp.float32), 1024.0)
    third = copies(2, 2, lambda j: out3.at[z ^ j], lambda j: in3.at[j])
    for c in third:
        c.start()
    seen = seen_by(2, *told[1])
    told.append((share(1, seen), seen))
    in3[0] = out3[z]
    for group in (first, second, told[0][0], told[1][0]):
        for c in group:
            c.wait_send()
    k = key_of(in3[0, 0], in3[0, 1])
    for j in reversed(FAR_FIRST[2]):
        third[FAR_FIRST[2].index(j)].wait_recv()
        k = jnp.maximum(k, key_of(in3[j, 0], in3[j, 1]))
    both[0] = jnp.where(k < 0, -1.0, (k >> 10).astype(jnp.float32) * (1.0 / 1024.0))
    both[1] = jnp.where(k < 0, -1, 1023 - (k & 1023)).astype(jnp.float32)
    flags[0, 0] = jnp.max(seen_by(1, *told[2])).astype(jnp.int32)
    for group in (third, told[2][0]):
        for c in group:
            c.wait_send()


def words(*shape):
    return pltpu.VMEM(shape + (8, 128), jnp.float32)


def sparse_path(cell, vehicle, speed):
    whole = pl.BlockSpec(memory_space=pltpu.VMEM)
    ints = lambda n: pltpu.VMEM((n, 8, 128), jnp.int32)
    return pl.pallas_call(
        exchange_kernel,
        out_shape=(
            jax.ShapeDtypeStruct((2, 8, 128), jnp.float32),
            jax.ShapeDtypeStruct((1, 1), jnp.int32),
        ),
        in_specs=[pl.BlockSpec(memory_space=pl.ANY)] * 3,
        out_specs=(whole, pl.BlockSpec(memory_space=pltpu.SMEM)),
        scratch_shapes=[
            pltpu.VMEM((2, 32, 8, 128), jnp.int32),
            words(32),
            ints(32),
            ints(32),
            words(8, 6),
            words(8, 6),
            pltpu.VMEM((8, 9, 4, 128), jnp.float32),
            pltpu.VMEM((8, 9, 4, 128), jnp.float32),
            words(8, 2),
            words(8, 2),
            pltpu.VMEM((3, 1, 128), jnp.float32),
            pltpu.VMEM((3, 8, 1, 128), jnp.float32),
            pltpu.SemaphoreType.DMA((3,)),
            pltpu.SemaphoreType.DMA((6, 8)),
            pltpu.SemaphoreType.DMA((6, 8)),
        ],
        compiler_params=pltpu.CompilerParams(collective_id=0, has_side_effects=True),
    )(cell, vehicle, speed)


def per_device(cell, vehicle, speed):
    shaped = [x.reshape(32, 8, 128) for x in (cell, vehicle, speed)]
    both, flags = sparse_path(*shaped)
    both = lax.cond(flags[0, 0] > 0, lambda: dense_path(cell, vehicle, speed), lambda: both)
    return both[0].reshape(1024), both[1].astype(jnp.int32).reshape(1024)


def solution(mesh):
    placed = (P(("gx", "gy")), P(("gx", "gy")), P(("gx", "gy")))
    return jax.shard_map(
        per_device,
        mesh=mesh,
        in_specs=placed,
        out_specs=(P(("gx", "gy")), P(("gx", "gy"))),
        check_vma=False,
    )
```
